256 devices in a mesh: tiles: 4 (over x, y), rows: 32 (over z), dates: 2 (over core).
Axes of the slice: x: 2, y: 2, z: 32, core: 2. Of those that a mesh axis runs over, the one named last changes fastest.
The devices are a block of a 4x8x32 slice.
Arguments:
- red_band: int32 [24, 4096, 2048], P('dates', ('tiles', 'rows')), parts along dimension 1, may hold values from 1 to 1073741823
- nir_band: int32 [24, 4096, 2048], P('dates', ('tiles', 'rows')), parts along dimension 1, may hold values from 1 to 1073741823
- cloud_class: int32 [24, 4096, 2048], P('dates', ('tiles', 'rows')), parts along dimension 1, may hold values from 0 to 3
- date_ordinal: int32 [96], P(('tiles', 'dates')), parts along dimension 0, may hold values from 0 to 23, each once
Outputs:
- composite_red: int32 [4096, 2048], P(('tiles', 'rows', 'dates')), parts along dimension 0
- composite_nir: int32 [4096, 2048], P(('tiles', 'rows', 'dates')), parts along dimension 0
- chosen_date: int32 [4096, 2048], P(('tiles', 'rows', 'dates')), parts along dimension 0
- overview_one: float32 [2, 2048, 1024], P(None, ('tiles', 'rows', 'dates')), parts along dimension 1
- overview_two: float32 [2, 1024, 512], P(None, ('tiles', 'rows', 'dates')), parts along dimension 1
- overview_three: float32 [2, 512, 256], P(None, ('tiles', 'rows', 'dates')), parts along dimension 1
The draws below stay inside these ranges and needn't reach their ends.
There are 4 independent parts, one for each index of `tiles`. The reference program is written for one: setup_inputs(seed, part) draws one part's arguments, and reference() takes and returns one part's arrays. A program takes and returns all parts, laid end to end along the dimension named above; each array names one. Nothing has to cross between parts.
Inputs may be any that keep to these rules, and one draw needn't show every extreme that they name: `date_ordinal`: each ordinal appears once.
All inputs are finite; a program needn't handle non-finite values.
Results may differ from the reference program's by a relative error of at most 0.0003.
Values sent between devices are 32-bit elements; how exact they have to be, the bound alone decides.
A program may use at most 192 MiB of HBM per device.

```python
import jax
import jax.numpy as jnp
from jax import lax

DATES = 24
W = 2048
LEVELS = 3
ROWS = 1024


def draw_bands(key):
    base = jax.random.fold_in(key, 7101)
    keys = jax.random.split(base, 10)
    shape = (DATES, ROWS, W)
    plane = (ROWS, W)
    free_red = jax.random.randint(keys[0], shape, 1, 1073741824, dtype=jnp.int32)
    free_nir = jax.random.randint(keys[1], shape, 1, 1073741824, dtype=jnp.int32)
    kind = jax.random.randint(keys[2], plane, 0, 4, dtype=jnp.int32)[None]
    joined_code = jax.random.randint(keys[3], shape, 0, 16, dtype=jnp.int32)
    joined = joined_code % 2 == 1
    offset = joined_code // 2
    pair = jax.random.randint(keys[4], plane, 0, 4, dtype=jnp.int32)[None]
    table_red = jnp.where(pair == 2, 2, 1).astype(jnp.int32)
    table_nir = jnp.where(pair == 0, 39, jnp.where(pair == 1, 49, jnp.where(pair == 2, 97, 99))).astype(jnp.int32)
    factor = jax.random.randint(keys[5], shape, 1, 10737418, dtype=jnp.int32)
    near_red = jax.random.randint(keys[6], plane, 16777216, 33554432, dtype=jnp.int32)[None]
    near_nir = jax.random.randint(keys[7], plane, 1006632960, 1073741808, dtype=jnp.int32)[None]
    copy_red = jax.random.randint(keys[8], plane, 4194304, 8388608, dtype=jnp.int32)[None]
    copy_nir = jax.random.randint(keys[9], plane, 536870912, 1073741824, dtype=jnp.int32)[None]
    red = jnp.where(joined & (kind == 1), table_red * factor, free_red)
    nir = jnp.where(joined & (kind == 1), table_nir * factor + offset, free_nir)
    red = jnp.where(joined & (kind == 2), near_red + offset, red)
    nir = jnp.where(joined & (kind == 2), near_nir + offset, nir)
    red = jnp.where(joined & (kind == 3), copy_red + jnp.zeros(shape, jnp.int32), red)
    nir = jnp.where(joined & (kind == 3), copy_nir + jnp.zeros(shape, jnp.int32), nir)
    return (red.astype(jnp.int32), nir.astype(jnp.int32))


def draw_red_band(key, part):
    return draw_bands(key)[0]


def draw_nir_band(key, part):
    return draw_bands(key)[1]


def place_ends(drawn, rng, smallest, high):
    index_at = [jax.random.randint(jax.random.fold_in(rng, axis), (), 0, length) for axis, length in enumerate(drawn.shape)]
    longest = drawn.shape.index(max(drawn.shape))
    beside = index_at[:longest] + [(index_at[longest] + 1) % drawn.shape[longest]] + index_at[longest + 1:]
    return drawn.at[tuple(index_at)].set(smallest).at[tuple(beside)].set(high)


def setup_inputs(seed: int = 0, part: int = 0) -> dict:
    key_list = jax.random.split(jax.random.key(seed), 5)
    part_splits = jax.random.split(jax.random.fold_in(key_list[4], part), 5)
    red_band = draw_red_band(jax.random.fold_in(jax.random.fold_in(key_list[4], part), 71), part)
    nir_band = draw_nir_band(jax.random.fold_in(jax.random.fold_in(key_list[4], part), 71), part)
    cloud_class = place_ends(jax.random.randint(part_splits[2], (DATES, ROWS, W), 0, 4), jax.random.fold_in(part_splits[2], 1), 0, 3).astype(jnp.int32)
    date_ordinal = jax.random.permutation(part_splits[3], DATES).astype(jnp.int32)
    return dict(red_band=red_band, nir_band=nir_band, cloud_class=cloud_class, date_ordinal=date_ordinal)


KERNEL = (0.0625, 0.25, 0.375, 0.25, 0.0625)
LIMB = 32768
TWO_LIMBS = 1073741824
SCALE_BAND = 9.313225746154785e-10


def product_digits(small, large):
    small_hi = small // LIMB
    small_lo = small % LIMB
    large_top = large // TWO_LIMBS
    remain = large % TWO_LIMBS
    large_mid = remain // LIMB
    large_lo = remain % LIMB
    digit_zero = small_lo * large_lo
    digit_one = small_hi * large_lo + small_lo * large_mid
    digit_two = small_hi * large_mid + small_lo * large_top
    digit_three = small_hi * large_top
    digit_one = digit_one + digit_zero // LIMB
    digit_zero = digit_zero % LIMB
    digit_two = digit_two + digit_one // LIMB
    digit_one = digit_one % LIMB
    digit_three = digit_three + digit_two // LIMB
    digit_two = digit_two % LIMB
    return (digit_three, digit_two, digit_one, digit_zero)


def compare_digits(first, second):
    greater = first[0] > second[0]
    equal = first[0] == second[0]
    for one, two in zip(first[1:], second[1:]):
        greater = greater | (equal & (one > two))
        equal = equal & (one == two)
    return greater, equal


def better(first, second):
    clear_a, red_a, nir_a, ord_a = first
    clear_b, red_b, nir_b, ord_b = second
    diff_a = nir_a - red_a
    diff_b = nir_b - red_b
    total_a = nir_a + red_a
    total_b = nir_b + red_b
    sign_a = jnp.sign(diff_a)
    sign_b = jnp.sign(diff_b)
    greater, equal = compare_digits(product_digits(jnp.abs(diff_a), total_b), product_digits(jnp.abs(diff_b), total_a))
    lesser = jnp.logical_not(greater | equal)
    same_sign = sign_a == sign_b
    ndvi_more = (sign_a > sign_b) | (same_sign & (((sign_a > 0) & greater) | ((sign_a < 0) & lesser)))
    ndvi_same = same_sign & ((sign_a == 0) | equal)
    same_clear = clear_a == clear_b
    take = (clear_a > clear_b) | (same_clear & (ndvi_more | (ndvi_same & (ord_a < ord_b))))
    return tuple(jnp.where(take, one, two) for one, two in zip(first, second))


def blur_pool(level):
    rows = level.shape[1]
    cols = level.shape[2]
    padded = jnp.pad(level, ((0, 0), (2, 2), (0, 0)))
    smooth = KERNEL[0] * padded[:, 0:rows]
    for offset in range(1, 5):
        smooth = smooth + KERNEL[offset] * padded[:, offset:offset + rows]
    padded = jnp.pad(smooth, ((0, 0), (0, 0), (2, 2)))
    result = KERNEL[0] * padded[:, :, 0:cols]
    for offset in range(1, 5):
        result = result + KERNEL[offset] * padded[:, :, offset:offset + cols]
    return result.reshape(2, rows // 2, 2, cols // 2, 2).mean(axis=(2, 4))


def reference(red_band, nir_band, cloud_class, date_ordinal):
    def entry(index):
        return ((cloud_class[index] == 0).astype(jnp.int32), red_band[index], nir_band[index],
                jnp.full(red_band.shape[1:], date_ordinal[index], jnp.int32))

    def advance(carry, index):
        return better(carry, entry(index)), None

    best, unused = lax.scan(advance, entry(0), jnp.arange(1, DATES, dtype=jnp.int32))
    level = jnp.stack([best[1], best[2]]).astype(jnp.float32) * SCALE_BAND
    levels = []
    for number in range(LEVELS):
        level = blur_pool(level)
        levels.append(level)
    return best[1], best[2], best[3], levels[0], levels[1], levels[2]
```

```python
import functools

import jax
import jax.numpy as jnp
from jax import lax
from jax.experimental import pallas as pl
from jax.experimental.pallas import tpu as pltpu
from jax.sharding import PartitionSpec as P

MESH = pl.DeviceIdType.MESH
LIMB_BITS = 15
LIMB_MASK = 32767
CLEAR = 1 << 30
FLAG_STEP = 32
SCALE_BAND = 9.313225746154785e-10
TAPS = (0.03125, 0.15625, 0.3125, 0.3125, 0.15625, 0.03125)
TILE = 8
GROUP = 512
SPAN = 256
WINDOW = 2 * SPAN + 256


def split(value):
    return value >> LIMB_BITS, value & LIMB_MASK


def join(high, low):
    return (high << LIMB_BITS) | low


def improve(best, new):
    n1, n0, r1, r0, clear, order = best
    m1, m0, s1, s0, fresh, index = new
    low = m0 * r0 - n0 * s0 + ((order - index) >> 31)
    mid = (m1 * r0 + m0 * r1) - (n1 * s0 + n0 * s1) + (low >> LIMB_BITS)
    top = m1 * r1 - n1 * s1 + (mid >> LIMB_BITS) + (fresh - clear)
    take = top >= 0
    return tuple(jnp.where(take, one, two) for one, two in zip(new, best))


def pooled(window, weights):
    parts = []
    for block in window:
        head = block.astype(jnp.bfloat16)
        parts += [head, (block - head.astype(jnp.float32)).astype(jnp.bfloat16)]
    rows = window[0].shape[0]
    out = jnp.dot(jnp.concatenate(parts, axis=0), weights, preferred_element_type=jnp.float32)
    return [out[2 * b * rows : (2 * b + 1) * rows] + out[(2 * b + 1) * rows : (2 * b + 2) * rows] for b in range(len(window))]


def kernel(
    ordinal, red, nir, cloud,
    comp_red, comp_nir, chosen, one, two, three,
    in_red, in_nir, in_cloud, sent, got, level, ext, weights, level1, ext1, level2, ext2,
    in_sem, send_sem, recv_sem, halo_send, halo_recv,
):
    dates, strip, cols = red.shape
    half = strip // 2
    tiles = half // TILE
    groups = cols // GROUP
    core = lax.axis_index("dates")
    z = lax.axis_index("rows")
    last = lax.axis_size("rows") - 1
    other = 1 - core
    has = jnp.where(core == 0, z > 0, z < last)
    beyond = jnp.where(core == 0, z - 1, z + 1)
    partner = {"dates": other}
    neighbour = {"rows": beyond, "dates": other}

    def tile_in_half(c, k):
        return jnp.where(c == 0, k, tiles - 1 - k)

    def loads(chunk):
        side = chunk // (tiles * groups)
        owner = jnp.where(side == 0, other, core)
        k = (chunk // groups) % tiles
        row = pl.multiple_of(owner * half + tile_in_half(owner, k) * TILE, TILE)
        col = pl.multiple_of((chunk % groups) * GROUP, GROUP)
        return [
            pltpu.make_async_copy(
                src.at[:, pl.ds(row, TILE), pl.ds(col, GROUP)], dst.at[chunk], in_sem.at[chunk, i]
            )
            for i, (src, dst) in enumerate(((red, in_red), (nir, in_nir), (cloud, in_cloud)))
        ]

    chunks = 2 * tiles * groups

    @pl.loop(0, chunks)
    def _(chunk):
        for copy in loads(chunk):
            copy.start()

    barrier = pltpu.get_barrier_semaphore()
    pl.semaphore_signal(barrier, inc=1, device_id=partner, device_id_type=MESH)

    @pl.when(has)
    def _():
        pl.semaphore_signal(barrier, inc=1, device_id=neighbour, device_id_type=MESH)

    shape = (WINDOW, SPAN)
    tap = lax.broadcasted_iota(jnp.int32, shape, 0) - 2 * lax.broadcasted_iota(jnp.int32, shape, 1) - 126
    factor = jnp.zeros(shape, jnp.float32)
    for i, weight in enumerate(TAPS):
        factor = jnp.where(tap == i, weight, factor)
    weights[...] = factor.astype(jnp.bfloat16)
    for buffer in (level, level1, level2):
        rows, width = buffer.shape
        buffer[:, 0:128] = jnp.zeros((rows, 128), jnp.float32)
        buffer[:, width - 128 :] = jnp.zeros((rows, 128), jnp.float32)
    lanes = ext.shape[0]
    ext[:, 0:8] = jnp.zeros((lanes, 8, 128), jnp.float32)
    ext[:, 56:64] = jnp.zeros((lanes, 8, 128), jnp.float32)

    @pl.when(jnp.logical_not(has))
    def _():
        edge = pl.multiple_of(jnp.where(core == 0, 8, 40), 8)
        ext[:, pl.ds(edge, half)] = jnp.zeros((lanes, half, 128), jnp.float32)

    def entry(chunk, d):
        m1, m0 = split(in_nir[chunk, d])
        s1, s0 = split(in_red[chunk, d])
        fresh = jnp.where(in_cloud[chunk, d] == 0, CLEAR, 0)
        return m1, m0, s1, s0, fresh, jnp.full((TILE, GROUP), ordinal[d], jnp.int32)

    def exchange(item):
        return pltpu.make_async_remote_copy(
            src_ref=sent.at[item],
            dst_ref=got.at[item],
            send_sem=send_sem.at[item],
            recv_sem=recv_sem.at[item],
            device_id=partner,
            device_id_type=MESH,
        )

    pl.semaphore_wait(barrier, jnp.where(has, 2, 1))

    @pl.loop(0, tiles * groups)
    def _(item):
        for copy in loads(item):
            copy.wait()
        best = entry(item, 0)
        for d in range(1, dates):
            best = improve(best, entry(item, d))
        n1, n0, r1, r0, clear, order = best
        sent[item, 0] = join(r1, r0)
        sent[item, 1] = join(n1, n0)
        sent[item, 2] = order + jnp.where(clear > 0, FLAG_STEP, 0)
        exchange(item).start()

    def halo(k, side):
        here = tile_in_half(core, k) * TILE
        there = 8 + 32 * (core if side == 0 else other) + here
        return pltpu.make_async_remote_copy(
            src_ref=ext.at[:, pl.ds(pl.multiple_of(24 + here, 8), TILE)],
            dst_ref=ext.at[:, pl.ds(pl.multiple_of(there, 8), TILE)],
            send_sem=halo_send.at[side, k],
            recv_sem=halo_recv.at[side, k],
            device_id=partner if side == 0 else neighbour,
            device_id_type=MESH,
        )

    @pl.loop(0, tiles)
    def _(k):
        row = pl.multiple_of(tile_in_half(core, k) * TILE, TILE)

        @pl.loop(0, groups)
        def _(g):
            item = k * groups + g
            chunk = tiles * groups + item
            for copy in loads(chunk):
                copy.wait()
            exchange(item).wait_recv()
            flagged = got[item, 2]
            is_clear = flagged >= FLAG_STEP
            best = (
                *split(got[item, 1]),
                *split(got[item, 0]),
                jnp.where(is_clear, CLEAR, 0),
                jnp.where(is_clear, flagged - FLAG_STEP, flagged),
            )
            for d in range(dates):
                best = improve(best, entry(chunk, d))
            n1, n0, r1, r0, _, order = best
            value_red, value_nir = join(r1, r0), join(n1, n0)
            col = pl.multiple_of(g * GROUP, GROUP)
            comp_red[pl.ds(row, TILE), pl.ds(col, GROUP)] = value_red
            comp_nir[pl.ds(row, TILE), pl.ds(col, GROUP)] = value_nir
            chosen[pl.ds(row, TILE), pl.ds(col, GROUP)] = order
            inner = pl.ds(pl.multiple_of(col + 128, 128), GROUP)
            level[0:8, inner] = value_red.astype(jnp.float32) * SCALE_BAND
            level[8:16, inner] = value_nir.astype(jnp.float32) * SCALE_BAND

        spans = cols // 2 // SPAN
        results = pooled([level[:, 2 * SPAN * b : 2 * SPAN * b + WINDOW] for b in range(spans)], weights[...])
        mine = pl.ds(pl.multiple_of(24 + row, 8), TILE)
        for b, result in enumerate(results):
            for i in range(SPAN // 128):
                piece = slice(i * 128, (i + 1) * 128)
                ext[b * (SPAN // 128) + i, mine] = result[0:8, piece]
                ext[lanes // 2 + b * (SPAN // 128) + i, mine] = result[8:16, piece]
        halo(k, 0).start()

        @pl.when(has)
        def _():
            halo(k, 1).start()

    for k in range(tiles):
        halo(k, 0).wait_recv()

    @pl.when(has)
    def _():
        for k in range(tiles):
            halo(k, 1).wait_recv()

    def inside(rows, near):
        index = lax.broadcasted_iota(jnp.int32, (rows, 128), 0)
        low = jnp.where(has | (core == 1), 0, near)
        high = jnp.where(has | (core == 0), rows, rows - near)
        return (index >= low) & (index < high)

    def stacked(source, block, start, rows):
        value = TAPS[0] * source[block, pl.ds(start, rows, 2), :]
        for i in range(1, 6):
            value = value + TAPS[i] * source[block, pl.ds(start + i, rows, 2), :]
        return value

    def descend(source, start, rows, keep, near, out, padded, target):
        valid = inside(rows, near)
        blocks = source.shape[0] // 2
        for band in range(2):
            for c in range(blocks):
                value = stacked(source, band * blocks + c, start, rows)
                out[band, :, c * 128 : (c + 1) * 128] = value[keep : keep + out.shape[1]]
                padded[band * rows : (band + 1) * rows, 128 * (c + 1) : 128 * (c + 2)] = jnp.where(valid, value, 0.0)
        spans = blocks * 64 // SPAN
        results = pooled([padded[:, 2 * SPAN * b : 2 * SPAN * b + WINDOW] for b in range(spans)], weights[...])
        for b, result in enumerate(results):
            for band in range(2):
                for i in range(SPAN // 128):
                    target[band * blocks // 2 + b * (SPAN // 128) + i] = result[
                        band * rows : (band + 1) * rows, i * 128 : (i + 1) * 128
                    ]

    descend(ext, 6, 24, 8, 8, one, level1, ext1)
    descend(ext1, 2, 8, 2, 2, two, level2, ext2)
    blocks = ext2.shape[0] // 2
    for band in range(2):
        for c in range(blocks):
            three[band, :, c * 128 : (c + 1) * 128] = stacked(ext2, band * blocks + c, 0, 2)

    @pl.loop(0, tiles * groups)
    def _(item):
        exchange(item).wait_send()

    for k in range(tiles):
        halo(k, 0).wait_send()

    @pl.when(has)
    def _():
        for k in range(tiles):
            halo(k, 1).wait_send()


def body(red_band, nir_band, cloud_class, date_ordinal):
    dates, strip, cols = red_band.shape
    half = strip // 2
    items = half // TILE * (cols // GROUP)
    whole = pl.BlockSpec(memory_space=pltpu.VMEM)
    far = pl.BlockSpec(memory_space=pltpu.HBM)
    f32, i32 = jnp.float32, jnp.int32
    return pl.pallas_call(
        kernel,
        out_shape=[jax.ShapeDtypeStruct((half, cols), i32)] * 3
        + [jax.ShapeDtypeStruct((2, half >> k, cols >> k), f32) for k in (1, 2, 3)],
        in_specs=[pl.BlockSpec(memory_space=pltpu.SMEM), far, far, far],
        out_specs=[whole] * 6,
        scratch_shapes=[pltpu.VMEM((2 * items, dates, TILE, GROUP), i32)] * 3
        + [
            pltpu.VMEM((items, 3, TILE, GROUP), i32),
            pltpu.VMEM((items, 3, TILE, GROUP), i32),
            pltpu.VMEM((16, cols + 256), f32),
            pltpu.VMEM((cols // 128, 64, 128), f32),
            pltpu.VMEM((WINDOW, SPAN), jnp.bfloat16),
            pltpu.VMEM((48, cols // 2 + 256), f32),
            pltpu.VMEM((cols // 256, 24, 128), f32),
            pltpu.VMEM((16, cols // 4 + 256), f32),
            pltpu.VMEM((cols // 512, 8, 128), f32),
            pltpu.SemaphoreType.DMA((2 * items, 3)),
            pltpu.SemaphoreType.DMA((items,)),
            pltpu.SemaphoreType.DMA((items,)),
            pltpu.SemaphoreType.DMA((2, half // TILE)),
            pltpu.SemaphoreType.DMA((2, half // TILE)),
        ],
        compiler_params=pltpu.CompilerParams(collective_id=0, has_side_effects=True),
        name="composite",
    )(date_ordinal, red_band, nir_band, cloud_class)


def solution(mesh):
    in_specs = (
        P("dates", ("tiles", "rows"), None),
        P("dates", ("tiles", "rows"), None),
        P("dates", ("tiles", "rows"), None),
        P(("tiles", "dates")),
    )
    out_specs = (
        P(("tiles", "rows", "dates"), None),
        P(("tiles", "rows", "dates"), None),
        P(("tiles", "rows", "dates"), None),
        P(None, ("tiles", "rows", "dates"), None),
        P(None, ("tiles", "rows", "dates"), None),
        P(None, ("tiles", "rows", "dates"), None),
    )
    return jax.shard_map(body, mesh=mesh, in_specs=in_specs, out_specs=out_specs, check_vma=False)
```

```python
import functools

import jax
import jax.numpy as jnp
from jax import lax
from jax.experimental import pallas as pl
from jax.experimental.pallas import tpu as pltpu
from jax.sharding import PartitionSpec as P

MESH = pl.DeviceIdType.MESH
LIMB_BITS = 15
LIMB_MASK = 32767
CLEAR = 1 << 30
FLAG_STEP = 32
SCALE_BAND = 9.313225746154785e-10
TAPS = (0.03125, 0.15625, 0.3125, 0.3125, 0.15625, 0.03125)
TILE = 8
GROUP = 512
SPAN = 256
WINDOW = 2 * SPAN + 256


def split(value):
    return value >> LIMB_BITS, value & LIMB_MASK


def join(high, low):
    return (high << LIMB_BITS) | low


def improve(best, new):
    n1, n0, r1, r0, clear, order = best
    m1, m0, s1, s0, fresh, index = new
    low = m0 * r0 - n0 * s0 + ((order - index) >> 31)
    mid = (m1 * r0 + m0 * r1) - (n1 * s0 + n0 * s1) + (low >> LIMB_BITS)
    top = m1 * r1 - n1 * s1 + (mid >> LIMB_BITS) + (fresh - clear)
    take = top >= 0
    return tuple(jnp.where(take, one, two) for one, two in zip(new, best))


def clear_margins(buffer):
    rows, width = buffer.shape
    buffer[:, 0:128] = jnp.zeros((rows, 128), jnp.float32)
    buffer[:, width - 128 :] = jnp.zeros((rows, 128), jnp.float32)


def pooled(window, weights):
    parts = []
    for block in window:
        head = block.astype(jnp.bfloat16)
        parts += [head, (block - head.astype(jnp.float32)).astype(jnp.bfloat16)]
    rows = window[0].shape[0]
    out = jnp.dot(jnp.concatenate(parts, axis=0), weights, preferred_element_type=jnp.float32)
    return [out[2 * b * rows : (2 * b + 1) * rows] + out[(2 * b + 1) * rows : (2 * b + 2) * rows] for b in range(len(window))]


def kernel(
    ordinal_far, red, nir, cloud,
    comp_red, comp_nir, chosen, ext, weights,
    ordinal, in_red, in_nir, in_cloud, sent, got, level,
    in_sem, ordinal_sem, send_sem, recv_sem, halo_send, halo_recv,
):
    dates, strip, cols = red.shape
    half = strip // 2
    tiles = half // TILE
    groups = cols // GROUP
    core = lax.axis_index("dates")
    z = lax.axis_index("rows")
    last = lax.axis_size("rows") - 1
    other = 1 - core
    has = jnp.where(core == 0, z > 0, z < last)
    beyond = jnp.where(core == 0, z - 1, z + 1)
    partner = {"dates": other}
    neighbour = {"rows": beyond, "dates": other}

    def tile_in_half(c, k):
        return jnp.where(c == 0, k, tiles - 1 - k)

    def loads(chunk):
        side = chunk // (tiles * groups)
        owner = jnp.where(side == 0, other, core)
        k = (chunk // groups) % tiles
        row = pl.multiple_of(owner * half + tile_in_half(owner, k) * TILE, TILE)
        col = pl.multiple_of((chunk % groups) * GROUP, GROUP)
        return [
            pltpu.make_async_copy(
                src.at[:, pl.ds(row, TILE), pl.ds(col, GROUP)], dst.at[chunk], in_sem.at[chunk, i]
            )
            for i, (src, dst) in enumerate(((red, in_red), (nir, in_nir), (cloud, in_cloud)))
        ]

    chunks = 2 * tiles * groups

    @pl.loop(0, chunks)
    def _(chunk):
        for copy in loads(chunk):
            copy.start()

    order_copy = pltpu.make_async_copy(ordinal_far, ordinal, ordinal_sem)
    order_copy.start()
    barrier = pltpu.get_barrier_semaphore()
    pl.semaphore_signal(barrier, inc=1, device_id=partner, device_id_type=MESH)

    @pl.when(has)
    def _():
        pl.semaphore_signal(barrier, inc=1, device_id=neighbour, device_id_type=MESH)

    shape = (WINDOW, SPAN)
    tap = lax.broadcasted_iota(jnp.int32, shape, 0) - 2 * lax.broadcasted_iota(jnp.int32, shape, 1) - 126
    factor = jnp.zeros(shape, jnp.float32)
    for i, weight in enumerate(TAPS):
        factor = jnp.where(tap == i, weight, factor)
    weights[...] = factor.astype(jnp.bfloat16)
    clear_margins(level)
    lanes = ext.shape[0]
    ext[:, 0:8] = jnp.zeros((lanes, 8, 128), jnp.float32)
    ext[:, 56:64] = jnp.zeros((lanes, 8, 128), jnp.float32)

    @pl.when(jnp.logical_not(has))
    def _():
        edge = pl.multiple_of(jnp.where(core == 0, 8, 40), 8)
        ext[:, pl.ds(edge, half)] = jnp.zeros((lanes, half, 128), jnp.float32)

    def entry(chunk, d):
        m1, m0 = split(in_nir[chunk, d])
        s1, s0 = split(in_red[chunk, d])
        fresh = jnp.where(in_cloud[chunk, d] == 0, CLEAR, 0)
        return m1, m0, s1, s0, fresh, jnp.full((TILE, GROUP), ordinal[d], jnp.int32)

    def exchange(item):
        return pltpu.make_async_remote_copy(
            src_ref=sent.at[item],
            dst_ref=got.at[item],
            send_sem=send_sem.at[item],
            recv_sem=recv_sem.at[item],
            device_id=partner,
            device_id_type=MESH,
        )

    order_copy.wait()
    pl.semaphore_wait(barrier, jnp.where(has, 2, 1))

    @pl.loop(0, tiles * groups)
    def _(item):
        for copy in loads(item):
            copy.wait()
        best = entry(item, 0)
        for d in range(1, dates):
            best = improve(best, entry(item, d))
        n1, n0, r1, r0, clear, order = best
        sent[item, 0] = join(r1, r0)
        sent[item, 1] = join(n1, n0)
        sent[item, 2] = order + jnp.where(clear > 0, FLAG_STEP, 0)
        exchange(item).start()

    def halo(k, side):
        here = tile_in_half(core, k) * TILE
        there = 8 + 32 * (core if side == 0 else other) + here
        return pltpu.make_async_remote_copy(
            src_ref=ext.at[:, pl.ds(pl.multiple_of(24 + here, 8), TILE)],
            dst_ref=ext.at[:, pl.ds(pl.multiple_of(there, 8), TILE)],
            send_sem=halo_send.at[side, k],
            recv_sem=halo_recv.at[side, k],
            device_id=partner if side == 0 else neighbour,
            device_id_type=MESH,
        )

    @pl.loop(0, tiles)
    def _(k):
        row = pl.multiple_of(tile_in_half(core, k) * TILE, TILE)

        @pl.loop(0, groups)
        def _(g):
            item = k * groups + g
            chunk = tiles * groups + item
            for copy in loads(chunk):
                copy.wait()
            exchange(item).wait_recv()
            flagged = got[item, 2]
            is_clear = flagged >= FLAG_STEP
            best = (
                *split(got[item, 1]),
                *split(got[item, 0]),
                jnp.where(is_clear, CLEAR, 0),
                jnp.where(is_clear, flagged - FLAG_STEP, flagged),
            )
            for d in range(dates):
                best = improve(best, entry(chunk, d))
            n1, n0, r1, r0, _, order = best
            value_red, value_nir = join(r1, r0), join(n1, n0)
            col = pl.multiple_of(g * GROUP, GROUP)
            comp_red[pl.ds(row, TILE), pl.ds(col, GROUP)] = value_red
            comp_nir[pl.ds(row, TILE), pl.ds(col, GROUP)] = value_nir
            chosen[pl.ds(row, TILE), pl.ds(col, GROUP)] = order
            inner = pl.ds(pl.multiple_of(col + 128, 128), GROUP)
            level[0:8, inner] = value_red.astype(jnp.float32) * SCALE_BAND
            level[8:16, inner] = value_nir.astype(jnp.float32) * SCALE_BAND

        spans = cols // 2 // SPAN
        results = pooled([level[:, 2 * SPAN * b : 2 * SPAN * b + WINDOW] for b in range(spans)], weights[...])
        mine = pl.ds(pl.multiple_of(24 + row, 8), TILE)
        for b, result in enumerate(results):
            for i in range(SPAN // 128):
                piece = slice(i * 128, (i + 1) * 128)
                ext[b * (SPAN // 128) + i, mine] = result[0:8, piece]
                ext[lanes // 2 + b * (SPAN // 128) + i, mine] = result[8:16, piece]
        halo(k, 0).start()

        @pl.when(has)
        def _():
            halo(k, 1).start()

    for k in range(tiles):
        halo(k, 0).wait_recv()

    @pl.when(has)
    def _():
        for k in range(tiles):
            halo(k, 1).wait_recv()

    @pl.loop(0, tiles * groups)
    def _(item):
        exchange(item).wait_send()

    for k in range(tiles):
        halo(k, 0).wait_send()

    @pl.when(has)
    def _():
        for k in range(tiles):
            halo(k, 1).wait_send()


def finish(
    comp_red, comp_nir, chosen, ext, weights,
    out_red, out_nir, out_chosen, out_one, out_two, out_three,
    level1, ext1, level2, ext2, one, two, three, sems,
):
    pairs = ((comp_red, out_red), (comp_nir, out_nir), (chosen, out_chosen), (one, out_one), (two, out_two), (three, out_three))
    copies = [pltpu.make_async_copy(src, dst, sems.at[i]) for i, (src, dst) in enumerate(pairs)]
    for copy in copies[:3]:
        copy.start()
    core = lax.axis_index("dates")
    z = lax.axis_index("rows")
    has = jnp.where(core == 0, z > 0, z < lax.axis_size("rows") - 1)
    clear_margins(level1)
    clear_margins(level2)

    def inside(rows, near):
        index = lax.broadcasted_iota(jnp.int32, (rows, 128), 0)
        low = jnp.where(has | (core == 1), 0, near)
        high = jnp.where(has | (core == 0), rows, rows - near)
        return (index >= low) & (index < high)

    def stacked(source, block, start, rows):
        value = TAPS[0] * source[block, pl.ds(start, rows, 2), :]
        for i in range(1, 6):
            value = value + TAPS[i] * source[block, pl.ds(start + i, rows, 2), :]
        return value

    def descend(source, start, rows, keep, near, out, padded, target):
        valid = inside(rows, near)
        blocks = source.shape[0] // 2
        for band in range(2):
            for c in range(blocks):
                value = stacked(source, band * blocks + c, start, rows)
                out[band, :, c * 128 : (c + 1) * 128] = value[keep : keep + out.shape[1]]
                padded[band * rows : (band + 1) * rows, 128 * (c + 1) : 128 * (c + 2)] = jnp.where(valid, value, 0.0)
        spans = blocks * 64 // SPAN
        results = pooled([padded[:, 2 * SPAN * b : 2 * SPAN * b + WINDOW] for b in range(spans)], weights[...])
        for b, result in enumerate(results):
            for band in range(2):
                for i in range(SPAN // 128):
                    target[band * blocks // 2 + b * (SPAN // 128) + i] = result[
                        band * rows : (band + 1) * rows, i * 128 : (i + 1) * 128
                    ]

    descend(ext, 6, 24, 8, 8, one, level1, ext1)
    copies[3].start()
    descend(ext1, 2, 8, 2, 2, two, level2, ext2)
    copies[4].start()
    blocks = ext2.shape[0] // 2
    for band in range(2):
        for c in range(blocks):
            three[band, :, c * 128 : (c + 1) * 128] = stacked(ext2, band * blocks + c, 0, 2)

    copies[5].start()
    for copy in copies:
        copy.wait()


def body(red_band, nir_band, cloud_class, date_ordinal):
    dates, strip, cols = red_band.shape
    half = strip // 2
    items = half // TILE * (cols // GROUP)
    whole = pl.BlockSpec(memory_space=pltpu.VMEM)
    far = pl.BlockSpec(memory_space=pltpu.HBM)
    f32, i32 = jnp.float32, jnp.int32
    arrays = (date_ordinal, red_band, nir_band, cloud_class)
    arrays = [pltpu.with_memory_space_constraint(array, pltpu.HBM) for array in arrays]
    near = pl.pallas_call(
        kernel,
        out_shape=[pltpu.VMEM((half, cols), i32)] * 3
        + [pltpu.VMEM((cols // 128, 64, 128), f32), pltpu.VMEM((WINDOW, SPAN), jnp.bfloat16)],
        in_specs=[far] * 4,
        out_specs=[whole] * 5,
        scratch_shapes=[pltpu.SMEM((dates,), i32)]
        + [pltpu.VMEM((2 * items, dates, TILE, GROUP), i32)] * 3
        + [
            pltpu.VMEM((items, 3, TILE, GROUP), i32),
            pltpu.VMEM((items, 3, TILE, GROUP), i32),
            pltpu.VMEM((16, cols + 256), f32),
            pltpu.SemaphoreType.DMA((2 * items, 3)),
            pltpu.SemaphoreType.DMA,
            pltpu.SemaphoreType.DMA((items,)),
            pltpu.SemaphoreType.DMA((items,)),
            pltpu.SemaphoreType.DMA((2, half // TILE)),
            pltpu.SemaphoreType.DMA((2, half // TILE)),
        ],
        compiler_params=pltpu.CompilerParams(
            collective_id=0, has_side_effects=True, vmem_limit_bytes=32 * 1024 * 1024
        ),
        name="composite",
    )(*arrays)
    levels = [(2, half >> k, cols >> k) for k in (1, 2, 3)]
    return pl.pallas_call(
        finish,
        out_shape=[jax.ShapeDtypeStruct((half, cols), i32)] * 3 + [jax.ShapeDtypeStruct(shape, f32) for shape in levels],
        in_specs=[whole] * 5,
        out_specs=[far] * 6,
        scratch_shapes=[
            pltpu.VMEM((48, cols // 2 + 256), f32),
            pltpu.VMEM((cols // 256, 24, 128), f32),
            pltpu.VMEM((16, cols // 4 + 256), f32),
            pltpu.VMEM((cols // 512, 8, 128), f32),
        ]
        + [pltpu.VMEM(shape, f32) for shape in levels]
        + [pltpu.SemaphoreType.DMA((6,))],
        compiler_params=pltpu.CompilerParams(vmem_limit_bytes=16 * 1024 * 1024),
        name="finish",
    )(*near)


def solution(mesh):
    in_specs = (
        P("dates", ("tiles", "rows"), None),
        P("dates", ("tiles", "rows"), None),
        P("dates", ("tiles", "rows"), None),
        P(("tiles", "dates")),
    )
    out_specs = (
        P(("tiles", "rows", "dates"), None),
        P(("tiles", "rows", "dates"), None),
        P(("tiles", "rows", "dates"), None),
        P(None, ("tiles", "rows", "dates"), None),
        P(None, ("tiles", "rows", "dates"), None),
        P(None, ("tiles", "rows", "dates"), None),
    )
    return jax.shard_map(body, mesh=mesh, in_specs=in_specs, out_specs=out_specs, check_vma=False)
```

```python
import functools

import jax
import jax.numpy as jnp
from jax import lax
from jax.experimental import pallas as pl
from jax.experimental.pallas import tpu as pltpu
from jax.sharding import PartitionSpec as P

MESH = pl.DeviceIdType.MESH
LIMB_BITS = 15
LIMB_MASK = 32767
CLEAR = 1 << 30
FLAG_STEP = 32
SCALE_BAND = 9.313225746154785e-10
TAPS = (0.03125, 0.15625, 0.3125, 0.3125, 0.15625, 0.03125)
TILE = 8
GROUP = 512
PART = 1024
SPAN = 256
WINDOW = 2 * SPAN + 256


def split(value):
    return value >> LIMB_BITS, value & LIMB_MASK


def join(high, low):
    return (high << LIMB_BITS) | low


def improve(best, new):
    n1, n0, r1, r0, clear, order = best
    m1, m0, s1, s0, fresh, index = new
    low = m0 * r0 - n0 * s0 + ((order - index) >> 31)
    mid = (m1 * r0 + m0 * r1) - (n1 * s0 + n0 * s1) + (low >> LIMB_BITS)
    top = m1 * r1 - n1 * s1 + (mid >> LIMB_BITS)
    take = top >= clear - fresh
    return tuple(jnp.where(take, one, two) for one, two in zip(new, best))


def clear_margins(buffer):
    rows, width = buffer.shape
    buffer[:, 0:128] = jnp.zeros((rows, 128), jnp.float32)
    buffer[:, width - 128 :] = jnp.zeros((rows, 128), jnp.float32)


def pooled(window, weights):
    parts = []
    for block in window:
        head = block.astype(jnp.bfloat16)
        parts += [head, (block - head.astype(jnp.float32)).astype(jnp.bfloat16)]
    rows = window[0].shape[0]
    out = jnp.dot(jnp.concatenate(parts, axis=0), weights, preferred_element_type=jnp.float32)
    return [out[2 * b * rows : (2 * b + 1) * rows] + out[(2 * b + 1) * rows : (2 * b + 2) * rows] for b in range(len(window))]


def kernel(
    ordinal_far, red, nir, cloud,
    comp_red, comp_nir, chosen, ext, weights,
    ordinal, in_red, in_nir, in_cloud, sent, got, level,
    in_sem, ordinal_sem, send_sem, recv_sem, halo_send, halo_recv,
):
    dates, strip, cols = red.shape
    half = strip // 2
    tiles = half // TILE
    core = lax.axis_index("dates")
    z = lax.axis_index("rows")
    last = lax.axis_size("rows") - 1
    other = 1 - core
    has = jnp.where(core == 0, z > 0, z < last)
    beyond = jnp.where(core == 0, z - 1, z + 1)
    partner = {"dates": other}
    neighbour = {"rows": beyond, "dates": other}

    def tile_in_half(c, k):
        return jnp.where(c == 0, k, tiles - 1 - k)

    def load(slot, part):
        owner = jnp.where(slot < tiles, other, core)
        row = pl.multiple_of(owner * half + tile_in_half(owner, slot % tiles) * TILE, TILE)
        col = pl.ds(part * PART, PART)
        return [
            pltpu.make_async_copy(src.at[:, pl.ds(row, TILE), col], dst.at[slot, :, :, col], in_sem.at[slot, part, i])
            for i, (src, dst) in enumerate(((red, in_red), (nir, in_nir), (cloud, in_cloud)))
        ]

    parts = cols // PART
    order_copy = pltpu.make_async_copy(ordinal_far, ordinal, ordinal_sem)
    order_copy.start()
    for slot in range(2 * tiles):
        for part in range(parts):
            for copy in load(slot, part):
                copy.start()

    barrier = pltpu.get_barrier_semaphore()
    pl.semaphore_signal(barrier, inc=1, device_id=partner, device_id_type=MESH)

    @pl.when(has)
    def _():
        pl.semaphore_signal(barrier, inc=1, device_id=neighbour, device_id_type=MESH)

    shape = (WINDOW, SPAN)
    tap = lax.broadcasted_iota(jnp.int32, shape, 0) - 2 * lax.broadcasted_iota(jnp.int32, shape, 1) - 126
    factor = jnp.zeros(shape, jnp.float32)
    for i, weight in enumerate(TAPS):
        factor = jnp.where(tap == i, weight, factor)
    weights[...] = factor.astype(jnp.bfloat16)
    clear_margins(level)
    lanes = ext.shape[0]
    ext[:, 0:8] = jnp.zeros((lanes, 8, 128), jnp.float32)
    ext[:, 56:64] = jnp.zeros((lanes, 8, 128), jnp.float32)

    @pl.when(jnp.logical_not(has))
    def _():
        edge = pl.multiple_of(jnp.where(core == 0, 8, 40), 8)
        ext[:, pl.ds(edge, half)] = jnp.zeros((lanes, half, 128), jnp.float32)

    def entry(slot, d, col):
        m1, m0 = split(in_nir[slot, d, :, col])
        s1, s0 = split(in_red[slot, d, :, col])
        fresh = jnp.where(in_cloud[slot, d, :, col] == 0, CLEAR, 0)
        return m1, m0, s1, s0, fresh, jnp.full((TILE, GROUP), ordinal[d], jnp.int32)

    def exchange(k):
        return pltpu.make_async_remote_copy(
            src_ref=sent.at[k],
            dst_ref=got.at[k],
            send_sem=send_sem.at[k],
            recv_sem=recv_sem.at[k],
            device_id=partner,
            device_id_type=MESH,
        )

    def offer(slot, col):
        best = entry(slot, 0, col)
        for d in range(1, dates):
            best = improve(best, entry(slot, d, col))
        n1, n0, r1, r0, clear, order = best
        sent[slot, 0, :, col] = join(r1, r0)
        sent[slot, 1, :, col] = join(n1, n0)
        sent[slot, 2, :, col] = order + jnp.where(clear > 0, FLAG_STEP, 0)

    def columns(start, count):
        return [pl.ds(start + i * GROUP, GROUP) for i in range(count // GROUP)]

    order_copy.wait()
    for part in range(parts):
        for copy in load(0, part):
            copy.wait()
        for col in columns(part * PART, PART):
            offer(0, col)
    pl.semaphore_wait(barrier, jnp.where(has, 2, 1))
    exchange(0).start()
    for slot in range(1, tiles):
        for part in range(parts):
            for copy in load(slot, part):
                copy.wait()
        for col in columns(0, cols):
            offer(slot, col)
        exchange(slot).start()

    def halo(k, side):
        here = tile_in_half(core, k) * TILE
        there = 8 + 32 * (core if side == 0 else other) + here
        return pltpu.make_async_remote_copy(
            src_ref=ext.at[:, pl.ds(pl.multiple_of(24 + here, 8), TILE)],
            dst_ref=ext.at[:, pl.ds(pl.multiple_of(there, 8), TILE)],
            send_sem=halo_send.at[side, k],
            recv_sem=halo_recv.at[side, k],
            device_id=partner if side == 0 else neighbour,
            device_id_type=MESH,
        )

    @pl.loop(0, tiles)
    def _(k):
        row = pl.multiple_of(tile_in_half(core, k) * TILE, TILE)
        slot = tiles + k
        for part in range(parts):
            for copy in load(slot, part):
                copy.wait()
        exchange(k).wait_recv()
        for col in columns(0, cols):
            flagged = got[k, 2, :, col]
            is_clear = flagged >= FLAG_STEP
            best = (
                *split(got[k, 1, :, col]),
                *split(got[k, 0, :, col]),
                jnp.where(is_clear, CLEAR, 0),
                jnp.where(is_clear, flagged - FLAG_STEP, flagged),
            )
            for d in range(dates):
                best = improve(best, entry(slot, d, col))
            n1, n0, r1, r0, _, order = best
            value_red, value_nir = join(r1, r0), join(n1, n0)
            comp_red[pl.ds(row, TILE), col] = value_red
            comp_nir[pl.ds(row, TILE), col] = value_nir
            chosen[pl.ds(row, TILE), col] = order
            inner = pl.ds(col.start + 128, GROUP)
            level[0:8, inner] = value_red.astype(jnp.float32) * SCALE_BAND
            level[8:16, inner] = value_nir.astype(jnp.float32) * SCALE_BAND

        spans = cols // 2 // SPAN
        results = pooled([level[:, 2 * SPAN * b : 2 * SPAN * b + WINDOW] for b in range(spans)], weights[...])
        mine = pl.ds(pl.multiple_of(24 + row, 8), TILE)
        for b, result in enumerate(results):
            for i in range(SPAN // 128):
                piece = slice(i * 128, (i + 1) * 128)
                ext[b * (SPAN // 128) + i, mine] = result[0:8, piece]
                ext[lanes // 2 + b * (SPAN // 128) + i, mine] = result[8:16, piece]
        halo(k, 0).start()

        @pl.when(has)
        def _():
            halo(k, 1).start()

    for k in range(tiles):
        halo(k, 0).wait_recv()

    @pl.when(has)
    def _():
        for k in range(tiles):
            halo(k, 1).wait_recv()

    for k in range(tiles):
        exchange(k).wait_send()
        halo(k, 0).wait_send()

    @pl.when(has)
    def _():
        for k in range(tiles):
            halo(k, 1).wait_send()


def finish(
    comp_red, comp_nir, chosen, ext, weights,
    out_red, out_nir, out_chosen, out_one, out_two, out_three,
    level1, ext1, level2, ext2, one, two, three, sems,
):
    pairs = ((comp_red, out_red), (comp_nir, out_nir), (chosen, out_chosen), (one, out_one), (two, out_two), (three, out_three))
    copies = [pltpu.make_async_copy(src, dst, sems.at[i]) for i, (src, dst) in enumerate(pairs)]
    for copy in copies[:3]:
        copy.start()
    core = lax.axis_index("dates")
    z = lax.axis_index("rows")
    has = jnp.where(core == 0, z > 0, z < lax.axis_size("rows") - 1)
    clear_margins(level1)
    clear_margins(level2)

    def inside(rows, near):
        index = lax.broadcasted_iota(jnp.int32, (rows, 128), 0)
        low = jnp.where(has | (core == 1), 0, near)
        high = jnp.where(has | (core == 0), rows, rows - near)
        return (index >= low) & (index < high)

    def stacked(source, block, start, rows):
        value = TAPS[0] * source[block, pl.ds(start, rows, 2), :]
        for i in range(1, 6):
            value = value + TAPS[i] * source[block, pl.ds(start + i, rows, 2), :]
        return value

    def descend(source, start, rows, keep, near, out, padded, target):
        valid = inside(rows, near)
        blocks = source.shape[0] // 2
        for band in range(2):
            for c in range(blocks):
                value = stacked(source, band * blocks + c, start, rows)
                out[band, :, c * 128 : (c + 1) * 128] = value[keep : keep + out.shape[1]]
                padded[band * rows : (band + 1) * rows, 128 * (c + 1) : 128 * (c + 2)] = jnp.where(valid, value, 0.0)
        spans = blocks * 64 // SPAN
        results = pooled([padded[:, 2 * SPAN * b : 2 * SPAN * b + WINDOW] for b in range(spans)], weights[...])
        for b, result in enumerate(results):
            for band in range(2):
                for i in range(SPAN // 128):
                    target[band * blocks // 2 + b * (SPAN // 128) + i] = result[
                        band * rows : (band + 1) * rows, i * 128 : (i + 1) * 128
                    ]

    descend(ext, 6, 24, 8, 8, one, level1, ext1)
    copies[3].start()
    descend(ext1, 2, 8, 2, 2, two, level2, ext2)
    copies[4].start()
    blocks = ext2.shape[0] // 2
    for band in range(2):
        for c in range(blocks):
            three[band, :, c * 128 : (c + 1) * 128] = stacked(ext2, band * blocks + c, 0, 2)

    copies[5].start()
    for copy in copies:
        copy.wait()


def body(red_band, nir_band, cloud_class, date_ordinal):
    dates, strip, cols = red_band.shape
    half = strip // 2
    tiles = half // TILE
    whole = pl.BlockSpec(memory_space=pltpu.VMEM)
    far = pl.BlockSpec(memory_space=pltpu.HBM)
    f32, i32 = jnp.float32, jnp.int32
    arrays = (date_ordinal, red_band, nir_band, cloud_class)
    arrays = [pltpu.with_memory_space_constraint(array, pltpu.HBM) for array in arrays]
    near = pl.pallas_call(
        kernel,
        out_shape=[pltpu.VMEM((half, cols), i32)] * 3
        + [pltpu.VMEM((cols // 128, 64, 128), f32), pltpu.VMEM((WINDOW, SPAN), jnp.bfloat16)],
        in_specs=[far] * 4,
        out_specs=[whole] * 5,
        scratch_shapes=[pltpu.SMEM((dates,), i32)]
        + [pltpu.VMEM((2 * tiles, dates, TILE, cols), i32)] * 3
        + [
            pltpu.VMEM((tiles, 3, TILE, cols), i32),
            pltpu.VMEM((tiles, 3, TILE, cols), i32),
            pltpu.VMEM((16, cols + 256), f32),
            pltpu.SemaphoreType.DMA((2 * tiles, cols // PART, 3)),
            pltpu.SemaphoreType.DMA,
            pltpu.SemaphoreType.DMA((tiles,)),
            pltpu.SemaphoreType.DMA((tiles,)),
            pltpu.SemaphoreType.DMA((2, tiles)),
            pltpu.SemaphoreType.DMA((2, tiles)),
        ],
        compiler_params=pltpu.CompilerParams(
            collective_id=0, has_side_effects=True, vmem_limit_bytes=32 * 1024 * 1024
        ),
        name="composite",
    )(*arrays)
    levels = [(2, half >> k, cols >> k) for k in (1, 2, 3)]
    return pl.pallas_call(
        finish,
        out_shape=[jax.ShapeDtypeStruct((half, cols), i32)] * 3 + [jax.ShapeDtypeStruct(shape, f32) for shape in levels],
        in_specs=[whole] * 5,
        out_specs=[far] * 6,
        scratch_shapes=[
            pltpu.VMEM((48, cols // 2 + 256), f32),
            pltpu.VMEM((cols // 256, 24, 128), f32),
            pltpu.VMEM((16, cols // 4 + 256), f32),
            pltpu.VMEM((cols // 512, 8, 128), f32),
        ]
        + [pltpu.VMEM(shape, f32) for shape in levels]
        + [pltpu.SemaphoreType.DMA((6,))],
        compiler_params=pltpu.CompilerParams(vmem_limit_bytes=16 * 1024 * 1024),
        name="finish",
    )(*near)


def solution(mesh):
    in_specs = (
        P("dates", ("tiles", "rows"), None),
        P("dates", ("tiles", "rows"), None),
        P("dates", ("tiles", "rows"), None),
        P(("tiles", "dates")),
    )
    out_specs = (
        P(("tiles", "rows", "dates"), None),
        P(("tiles", "rows", "dates"), None),
        P(("tiles", "rows", "dates"), None),
        P(None, ("tiles", "rows", "dates"), None),
        P(None, ("tiles", "rows", "dates"), None),
        P(None, ("tiles", "rows", "dates"), None),
    )
    return jax.shard_map(body, mesh=mesh, in_specs=in_specs, out_specs=out_specs, check_vma=False)
```

```python
import functools

import jax
import jax.numpy as jnp
from jax import lax
from jax.experimental import pallas as pl
from jax.experimental.pallas import tpu as pltpu
from jax.sharding import PartitionSpec as P

MESH = pl.DeviceIdType.MESH
LIMB_BITS = 15
LIMB_MASK = 32767
CLEAR = 1 << 30
FLAG_STEP = 32
SCALE_BAND = 9.313225746154785e-10
TAPS = (0.03125, 0.15625, 0.3125, 0.3125, 0.15625, 0.03125)
TILE = 8
GROUP = 512
PART = 1024
SPAN = 256
WINDOW = 2 * SPAN + 256


def split(value):
    return value >> LIMB_BITS, value & LIMB_MASK


def join(high, low):
    return (high << LIMB_BITS) | low


def improve(best, new):
    n1, n0, r1, r0, clear, order = best
    m1, m0, s1, s0, fresh, index = new
    low = m0 * r0 - n0 * s0 + ((order - index) >> 31)
    mid = (m1 * r0 + m0 * r1) - (n1 * s0 + n0 * s1) + (low >> LIMB_BITS)
    top = m1 * r1 - n1 * s1 + (mid >> LIMB_BITS)
    take = top >= clear - fresh
    return tuple(jnp.where(take, one, two) for one, two in zip(new, best))


def clear_margins(buffer):
    rows, width = buffer.shape
    buffer[:, 0:128] = jnp.zeros((rows, 128), jnp.float32)
    buffer[:, width - 128 :] = jnp.zeros((rows, 128), jnp.float32)


def pooled(window, weights):
    parts = []
    for block in window:
        head = block.astype(jnp.bfloat16)
        parts += [head, (block - head.astype(jnp.float32)).astype(jnp.bfloat16)]
    rows = window[0].shape[0]
    out = jnp.dot(jnp.concatenate(parts, axis=0), weights, preferred_element_type=jnp.float32)
    return [out[2 * b * rows : (2 * b + 1) * rows] + out[(2 * b + 1) * rows : (2 * b + 2) * rows] for b in range(len(window))]


def kernel(
    ordinal_far, red, nir, cloud,
    comp, ext, weights,
    ordinal, images, sent, got, mine, level,
    in_sem, ordinal_sem, send_sem, recv_sem, halo_send, halo_recv,
):
    dates, strip, cols = red.shape
    half = strip // 2
    tiles = half // TILE
    core = lax.axis_index("dates")
    z = lax.axis_index("rows")
    last = lax.axis_size("rows") - 1
    other = 1 - core
    has = jnp.where(core == 0, z > 0, z < last)
    beyond = jnp.where(core == 0, z - 1, z + 1)
    partner = {"dates": other}
    neighbour = {"rows": beyond, "dates": other}

    def tile_in_half(c, k):
        return jnp.where(c == 0, k, tiles - 1 - k)

    pieces = [(0, part, PART) for part in range(0, cols, PART)] + [(slot, 0, cols) for slot in range(1, 2 * tiles)]

    def load(i):
        slot, start, width = pieces[i]
        owner = other if slot < tiles else core
        row = pl.multiple_of(owner * half + tile_in_half(owner, slot % tiles) * TILE, TILE)
        col = pl.ds(start, width)
        for j, src in enumerate((red, nir, cloud)):
            pltpu.make_async_copy(src.at[:, pl.ds(row, TILE), col], images.at[slot, j, :, :, col], in_sem.at[i]).start()

    def loaded(i):
        slot, start, width = pieces[i]
        there = images.at[slot, :, :, :, pl.ds(start, width)]
        pltpu.make_async_copy(there, there, in_sem.at[i]).wait()

    order_copy = pltpu.make_async_copy(ordinal_far, ordinal, ordinal_sem)
    order_copy.start()
    for i in range(len(pieces)):
        load(i)

    barrier = pltpu.get_barrier_semaphore()
    pl.semaphore_signal(barrier, inc=1, device_id=partner, device_id_type=MESH)

    @pl.when(has)
    def _():
        pl.semaphore_signal(barrier, inc=1, device_id=neighbour, device_id_type=MESH)

    shape = (WINDOW, SPAN)
    tap = lax.broadcasted_iota(jnp.int32, shape, 0) - 2 * lax.broadcasted_iota(jnp.int32, shape, 1) - 126
    factor = jnp.zeros(shape, jnp.float32)
    for i, weight in enumerate(TAPS):
        factor = jnp.where(tap == i, weight, factor)
    weights[...] = factor.astype(jnp.bfloat16)
    clear_margins(level)
    lanes = ext.shape[0]
    ext[:, 0:8] = jnp.zeros((lanes, 8, 128), jnp.float32)
    ext[:, 56:64] = jnp.zeros((lanes, 8, 128), jnp.float32)

    @pl.when(jnp.logical_not(has))
    def _():
        edge = pl.multiple_of(jnp.where(core == 0, 8, 40), 8)
        ext[:, pl.ds(edge, half)] = jnp.zeros((lanes, half, 128), jnp.float32)

    def entry(slot, d, col):
        m1, m0 = split(images[slot, 1, d, :, col])
        s1, s0 = split(images[slot, 0, d, :, col])
        fresh = jnp.where(images[slot, 2, d, :, col] == 0, CLEAR, 0)
        return m1, m0, s1, s0, fresh, jnp.full((TILE, GROUP), ordinal[d], jnp.int32)

    def exchange(k):
        return pltpu.make_async_remote_copy(
            src_ref=sent.at[k],
            dst_ref=got.at[k],
            send_sem=send_sem,
            recv_sem=recv_sem.at[k],
            device_id=partner,
            device_id_type=MESH,
        )

    def columns(start, count):
        return [pl.ds(start + i * GROUP, GROUP) for i in range(count // GROUP)]

    def best_of(slot, col):
        best = entry(slot, 0, col)
        for d in range(1, dates):
            best = improve(best, entry(slot, d, col))
        return best

    def offer(slot, col):
        n1, n0, r1, r0, clear, order = best_of(slot, col)
        sent[slot, 0, :, col] = join(r1, r0)
        sent[slot, 1, :, col] = join(n1, n0)
        sent[slot, 2, :, col] = order + jnp.where(clear > 0, FLAG_STEP, 0)

    order_copy.wait()
    for i, (slot, start, width) in enumerate(pieces):
        if slot < tiles:
            loaded(i)
            for col in columns(start, width):
                offer(slot, col)
            if start + width == cols:
                if slot == 0:
                    pl.semaphore_wait(barrier, jnp.where(has, 2, 1))
                exchange(slot).start()

    base = len(pieces) - tiles
    for k in range(tiles):
        loaded(base + k)
        for col in columns(0, cols):
            for i, limb in enumerate(best_of(tiles + k, col)):
                mine[k, i, :, col] = limb

    def halo(k, side):
        here = tile_in_half(core, k) * TILE
        there = 8 + 32 * (core if side == 0 else other) + here
        return pltpu.make_async_remote_copy(
            src_ref=ext.at[:, pl.ds(pl.multiple_of(24 + here, 8), TILE)],
            dst_ref=ext.at[:, pl.ds(pl.multiple_of(there, 8), TILE)],
            send_sem=halo_send.at[side],
            recv_sem=halo_recv.at[side],
            device_id=partner if side == 0 else neighbour,
            device_id_type=MESH,
        )

    def settle(k):
        row = pl.multiple_of(tile_in_half(core, k) * TILE, TILE)
        for col in columns(0, cols):
            flagged = got[k, 2, :, col]
            is_clear = flagged >= FLAG_STEP
            theirs = (
                *split(got[k, 1, :, col]),
                *split(got[k, 0, :, col]),
                jnp.where(is_clear, CLEAR, 0),
                jnp.where(is_clear, flagged - FLAG_STEP, flagged),
            )
            n1, n0, r1, r0, _, order = improve(tuple(mine[k, i, :, col] for i in range(6)), theirs)
            value_red, value_nir = join(r1, r0), join(n1, n0)
            comp[0, pl.ds(row, TILE), col] = value_red
            comp[1, pl.ds(row, TILE), col] = value_nir
            comp[2, pl.ds(row, TILE), col] = order
            inner = pl.ds(col.start + 128, GROUP)
            level[0:8, inner] = value_red.astype(jnp.float32) * SCALE_BAND
            level[8:16, inner] = value_nir.astype(jnp.float32) * SCALE_BAND

        spans = cols // 2 // SPAN
        results = pooled([level[:, 2 * SPAN * b : 2 * SPAN * b + WINDOW] for b in range(spans)], weights[...])
        here = pl.ds(pl.multiple_of(24 + row, 8), TILE)
        for b, result in enumerate(results):
            for i in range(SPAN // 128):
                piece = slice(i * 128, (i + 1) * 128)
                ext[b * (SPAN // 128) + i, here] = result[0:8, piece]
                ext[lanes // 2 + b * (SPAN // 128) + i, here] = result[8:16, piece]

    for k in range(tiles):
        exchange(k).wait_recv()
        settle(k)
        halo(k, 0).start()

        @pl.when(has)
        def _():
            halo(k, 1).start()

    def settled(sems, side):
        both = ext.at[:, 8 : 8 + half]
        pltpu.make_async_copy(both, both, sems.at[side]).wait()

    settled(halo_recv, 0)

    @pl.when(has)
    def _():
        settled(halo_recv, 1)

    pltpu.make_async_copy(sent, sent, send_sem).wait()
    settled(halo_send, 0)

    @pl.when(has)
    def _():
        settled(halo_send, 1)


def finish(
    comp, ext, weights,
    out_red, out_nir, out_chosen, out_one, out_two, out_three,
    level1, ext1, level2, ext2, one, two, three, comp_sem, sems,
):
    for i, out in enumerate((out_red, out_nir, out_chosen)):
        pltpu.make_async_copy(comp.at[i], out, comp_sem).start()
    pairs = ((one, out_one), (two, out_two), (three, out_three))
    copies = [pltpu.make_async_copy(src, dst, sems.at[i]) for i, (src, dst) in enumerate(pairs)]
    core = lax.axis_index("dates")
    z = lax.axis_index("rows")
    has = jnp.where(core == 0, z > 0, z < lax.axis_size("rows") - 1)
    clear_margins(level1)
    clear_margins(level2)

    def inside(rows, near):
        index = lax.broadcasted_iota(jnp.int32, (rows, 128), 0)
        low = jnp.where(has | (core == 1), 0, near)
        high = jnp.where(has | (core == 0), rows, rows - near)
        return (index >= low) & (index < high)

    def stacked(source, block, start, rows):
        value = TAPS[0] * source[block, pl.ds(start, rows, 2), :]
        for i in range(1, 6):
            value = value + TAPS[i] * source[block, pl.ds(start + i, rows, 2), :]
        return value

    def descend(source, start, rows, keep, near, out, padded, target):
        valid = inside(rows, near)
        blocks = source.shape[0] // 2
        for band in range(2):
            for c in range(blocks):
                value = stacked(source, band * blocks + c, start, rows)
                out[band, :, c * 128 : (c + 1) * 128] = value[keep : keep + out.shape[1]]
                padded[band * rows : (band + 1) * rows, 128 * (c + 1) : 128 * (c + 2)] = jnp.where(valid, value, 0.0)
        spans = blocks * 64 // SPAN
        results = pooled([padded[:, 2 * SPAN * b : 2 * SPAN * b + WINDOW] for b in range(spans)], weights[...])
        for b, result in enumerate(results):
            for band in range(2):
                for i in range(SPAN // 128):
                    target[band * blocks // 2 + b * (SPAN // 128) + i] = result[
                        band * rows : (band + 1) * rows, i * 128 : (i + 1) * 128
                    ]

    descend(ext, 6, 24, 8, 8, one, level1, ext1)
    copies[0].start()
    descend(ext1, 2, 8, 2, 2, two, level2, ext2)
    copies[1].start()
    blocks = ext2.shape[0] // 2
    for band in range(2):
        for c in range(blocks):
            three[band, :, c * 128 : (c + 1) * 128] = stacked(ext2, band * blocks + c, 0, 2)

    copies[2].start()
    for copy in copies:
        copy.wait()
    pltpu.make_async_copy(comp, comp, comp_sem).wait()


def body(red_band, nir_band, cloud_class, date_ordinal):
    dates, strip, cols = red_band.shape
    half = strip // 2
    tiles = half // TILE
    whole = pl.BlockSpec(memory_space=pltpu.VMEM)
    far = pl.BlockSpec(memory_space=pltpu.HBM)
    f32, i32 = jnp.float32, jnp.int32
    arrays = (date_ordinal, red_band, nir_band, cloud_class)
    arrays = [pltpu.with_memory_space_constraint(array, pltpu.HBM) for array in arrays]
    near = pl.pallas_call(
        kernel,
        out_shape=[
            pltpu.VMEM((3, half, cols), i32),
            pltpu.VMEM((cols // 128, 64, 128), f32),
            pltpu.VMEM((WINDOW, SPAN), jnp.bfloat16),
        ],
        in_specs=[far] * 4,
        out_specs=[whole] * 3,
        scratch_shapes=[
            pltpu.SMEM((dates,), i32),
            pltpu.VMEM((2 * tiles, 3, dates, TILE, cols), i32),
            pltpu.VMEM((tiles, 3, TILE, cols), i32),
            pltpu.VMEM((tiles, 3, TILE, cols), i32),
            pltpu.VMEM((tiles, 6, TILE, cols), i32),
            pltpu.VMEM((16, cols + 256), f32),
            pltpu.SemaphoreType.DMA((cols // PART + 2 * tiles - 1,)),
            pltpu.SemaphoreType.DMA,
            pltpu.SemaphoreType.DMA,
            pltpu.SemaphoreType.DMA((tiles,)),
            pltpu.SemaphoreType.DMA((2,)),
            pltpu.SemaphoreType.DMA((2,)),
        ],
        compiler_params=pltpu.CompilerParams(
            collective_id=0, has_side_effects=True, vmem_limit_bytes=32 * 1024 * 1024
        ),
        name="composite",
    )(*arrays)
    levels = [(2, half >> k, cols >> k) for k in (1, 2, 3)]
    return pl.pallas_call(
        finish,
        out_shape=[jax.ShapeDtypeStruct((half, cols), i32)] * 3 + [jax.ShapeDtypeStruct(shape, f32) for shape in levels],
        in_specs=[whole] * 3,
        out_specs=[far] * 6,
        scratch_shapes=[
            pltpu.VMEM((48, cols // 2 + 256), f32),
            pltpu.VMEM((cols // 256, 24, 128), f32),
            pltpu.VMEM((16, cols // 4 + 256), f32),
            pltpu.VMEM((cols // 512, 8, 128), f32),
        ]
        + [pltpu.VMEM(shape, f32) for shape in levels]
        + [pltpu.SemaphoreType.DMA, pltpu.SemaphoreType.DMA((3,))],
        compiler_params=pltpu.CompilerParams(vmem_limit_bytes=16 * 1024 * 1024),
        name="finish",
    )(*near)


def solution(mesh):
    in_specs = (
        P("dates", ("tiles", "rows"), None),
        P("dates", ("tiles", "rows"), None),
        P("dates", ("tiles", "rows"), None),
        P(("tiles", "dates")),
    )
    out_specs = (
        P(("tiles", "rows", "dates"), None),
        P(("tiles", "rows", "dates"), None),
        P(("tiles", "rows", "dates"), None),
        P(None, ("tiles", "rows", "dates"), None),
        P(None, ("tiles", "rows", "dates"), None),
        P(None, ("tiles", "rows", "dates"), None),
    )
    return jax.shard_map(body, mesh=mesh, in_specs=in_specs, out_specs=out_specs, check_vma=False)
```

```python
import functools

import jax
import jax.numpy as jnp
from jax import lax
from jax.experimental import pallas as pl
from jax.experimental.pallas import tpu as pltpu
from jax.sharding import PartitionSpec as P

MESH = pl.DeviceIdType.MESH
LIMB_BITS = 15
LIMB_MASK = 32767
CLEAR = 1 << 30
FLAG_STEP = 32
SCALE_BAND = 9.313225746154785e-10
TAPS = (0.03125, 0.15625, 0.3125, 0.3125, 0.15625, 0.03125)
TILE = 8
GROUP = 512
SPAN = 256
WINDOW = 2 * SPAN + 256


def split(value):
    return value >> LIMB_BITS, value & LIMB_MASK


def join(high, low):
    return (high << LIMB_BITS) | low


def improve(best, new, bar):
    n1, n0, r1, r0, order = best
    m1, m0, s1, s0, index = new
    low = m0 * r0 - n0 * s0 + ((order - index) >> 31)
    mid = (m1 * r0 + m0 * r1) - (n1 * s0 + n0 * s1) + (low >> LIMB_BITS)
    take = m1 * r1 - n1 * s1 + (mid >> LIMB_BITS) >= bar
    return tuple(jnp.where(take, one, two) for one, two in zip(new, best))


def clear_margins(buffer):
    rows, width = buffer.shape
    buffer[:, 0:128] = jnp.zeros((rows, 128), jnp.float32)
    buffer[:, width - 128 :] = jnp.zeros((rows, 128), jnp.float32)


def pooled(window, weights):
    parts = []
    for block in window:
        head = block.astype(jnp.bfloat16)
        parts += [head, (block - head.astype(jnp.float32)).astype(jnp.bfloat16)]
    rows = window[0].shape[0]
    out = jnp.dot(jnp.concatenate(parts, axis=0), weights, preferred_element_type=jnp.float32)
    return [out[2 * b * rows : (2 * b + 1) * rows] + out[(2 * b + 1) * rows : (2 * b + 2) * rows] for b in range(len(window))]


def pieces_of(tiles, cols):
    half = cols // 2
    first = [(0, 0, GROUP), (0, GROUP, half - GROUP), (0, half, half), (1, 0, half), (1, half, half)]
    return first + [(slot, 0, cols) for slot in range(2, 2 * tiles)]


def kernel(
    ordinal_far, red, nir, cloud,
    comp, ext, weights,
    ordinal, images, sent, got, mine, level,
    in_sem, ordinal_sem, send_sem, recv_sem, halo_send, halo_recv,
):
    dates, strip, cols = red.shape
    half = strip // 2
    tiles = half // TILE
    core = lax.axis_index("dates")
    z = lax.axis_index("rows")
    last = lax.axis_size("rows") - 1
    other = 1 - core
    has = jnp.where(core == 0, z > 0, z < last)
    beyond = jnp.where(core == 0, z - 1, z + 1)
    partner = {"dates": other}
    neighbour = {"rows": beyond, "dates": other}

    def tile_in_half(c, k):
        return jnp.where(c == 0, k, tiles - 1 - k)

    pieces = pieces_of(tiles, cols)

    def load(i):
        slot, start, width = pieces[i]
        owner = other if slot < tiles else core
        row = pl.multiple_of(owner * half + tile_in_half(owner, slot % tiles) * TILE, TILE)
        col = pl.ds(start, width)
        for j, src in enumerate((red, nir, cloud)):
            pltpu.make_async_copy(src.at[:, pl.ds(row, TILE), col], images.at[slot, j, :, :, col], in_sem.at[i]).start()

    def loaded(i):
        slot, start, width = pieces[i]
        there = images.at[slot, :, :, :, pl.ds(start, width)]
        pltpu.make_async_copy(there, there, in_sem.at[i]).wait()

    order_copy = pltpu.make_async_copy(ordinal_far, ordinal, ordinal_sem)
    order_copy.start()
    for i in range(len(pieces)):
        load(i)

    barrier = pltpu.get_barrier_semaphore()
    pl.semaphore_signal(barrier, inc=1, device_id=partner, device_id_type=MESH)

    @pl.when(has)
    def _():
        pl.semaphore_signal(barrier, inc=1, device_id=neighbour, device_id_type=MESH)

    shape = (WINDOW, SPAN)
    tap = lax.broadcasted_iota(jnp.int32, shape, 0) - 2 * lax.broadcasted_iota(jnp.int32, shape, 1) - 126
    factor = jnp.zeros(shape, jnp.float32)
    for i, weight in enumerate(TAPS):
        factor = jnp.where(tap == i, weight, factor)
    weights[...] = factor.astype(jnp.bfloat16)
    for k in range(tiles):
        clear_margins(level.at[k])
    lanes = ext.shape[0]
    ext[:, 0:8] = jnp.zeros((lanes, 8, 128), jnp.float32)
    ext[:, 56:64] = jnp.zeros((lanes, 8, 128), jnp.float32)

    @pl.when(jnp.logical_not(has))
    def _():
        edge = pl.multiple_of(jnp.where(core == 0, 8, 40), 8)
        ext[:, pl.ds(edge, half)] = jnp.zeros((lanes, half, 128), jnp.float32)

    def best_of(slot, col):
        lowest = images[slot, 2, 0, :, col]
        for d in range(1, dates):
            lowest = jnp.minimum(lowest, images[slot, 2, d, :, col])
        limit = jnp.where(lowest == 0, 0, CLEAR)
        best = None
        for d in range(dates):
            nir_value = jnp.where(images[slot, 2, d, :, col] > limit, 0, images[slot, 1, d, :, col])
            order = jnp.full((TILE, GROUP), ordinal[d], jnp.int32)
            new = (*split(nir_value), *split(images[slot, 0, d, :, col]), order)
            best = new if best is None else improve(best, new, 0)
        return best, lowest == 0

    def exchange(k):
        return pltpu.make_async_remote_copy(
            src_ref=sent.at[k],
            dst_ref=got.at[k],
            send_sem=send_sem,
            recv_sem=recv_sem.at[k],
            device_id=partner,
            device_id_type=MESH,
        )

    def columns(start, count):
        return [pl.ds(start + i * GROUP, GROUP) for i in range(count // GROUP)]

    def offer(slot, col):
        (n1, n0, r1, r0, order), is_clear = best_of(slot, col)
        sent[slot, 0, :, col] = join(r1, r0)
        sent[slot, 1, :, col] = join(n1, n0)
        sent[slot, 2, :, col] = order + jnp.where(is_clear, FLAG_STEP, 0)

    order_copy.wait()
    for i, (slot, start, width) in enumerate(pieces):
        if slot < tiles:
            loaded(i)
            for col in columns(start, width):
                offer(slot, col)
            if start + width == cols:
                if slot == 0:
                    pl.semaphore_wait(barrier, jnp.where(has, 2, 1))
                exchange(slot).start()

    base = len(pieces) - tiles
    for k in range(tiles):
        loaded(base + k)
        for col in columns(0, cols):
            best, is_clear = best_of(tiles + k, col)
            for i, limb in enumerate((*best, jnp.where(is_clear, CLEAR, 0))):
                mine[k, i, :, col] = limb

    def halo(k, side):
        here = tile_in_half(core, k) * TILE
        there = 8 + 32 * (core if side == 0 else other) + here
        return pltpu.make_async_remote_copy(
            src_ref=ext.at[:, pl.ds(pl.multiple_of(24 + here, 8), TILE)],
            dst_ref=ext.at[:, pl.ds(pl.multiple_of(there, 8), TILE)],
            send_sem=halo_send.at[side],
            recv_sem=halo_recv.at[side],
            device_id=partner if side == 0 else neighbour,
            device_id_type=MESH,
        )

    def settle(k):
        row = pl.multiple_of(tile_in_half(core, k) * TILE, TILE)
        for col in columns(0, cols):
            flagged = got[k, 2, :, col]
            is_clear = flagged >= FLAG_STEP
            order = jnp.where(is_clear, flagged - FLAG_STEP, flagged)
            theirs = (*split(got[k, 1, :, col]), *split(got[k, 0, :, col]), order)
            bar = mine[k, 5, :, col] - jnp.where(is_clear, CLEAR, 0)
            n1, n0, r1, r0, order = improve(tuple(mine[k, i, :, col] for i in range(5)), theirs, bar)
            value_red, value_nir = join(r1, r0), join(n1, n0)
            comp[0, pl.ds(row, TILE), col] = value_red
            comp[1, pl.ds(row, TILE), col] = value_nir
            comp[2, pl.ds(row, TILE), col] = order
            inner = pl.ds(col.start + 128, GROUP)
            level[k, 0:8, inner] = value_red.astype(jnp.float32) * SCALE_BAND
            level[k, 8:16, inner] = value_nir.astype(jnp.float32) * SCALE_BAND

    def narrow(k):
        spans = cols // 2 // SPAN
        results = pooled([level[k, :, 2 * SPAN * b : 2 * SPAN * b + WINDOW] for b in range(spans)], weights[...])
        here = pl.ds(pl.multiple_of(24 + tile_in_half(core, k) * TILE, 8), TILE)
        for b, result in enumerate(results):
            for i in range(SPAN // 128):
                piece = slice(i * 128, (i + 1) * 128)
                ext[b * (SPAN // 128) + i, here] = result[0:8, piece]
                ext[lanes // 2 + b * (SPAN // 128) + i, here] = result[8:16, piece]

    for k in range(tiles):
        exchange(k).wait_recv()
    for k in range(tiles):
        settle(k)
        narrow(k)
    for side in range(2):

        @pl.when((side == 0) | has)
        def _():
            for k in range(tiles):
                halo(k, side).start()

    def settled(sems, side):
        both = ext.at[:, 8 : 8 + half]
        pltpu.make_async_copy(both, both, sems.at[side]).wait()

    settled(halo_recv, 0)

    @pl.when(has)
    def _():
        settled(halo_recv, 1)

    pltpu.make_async_copy(sent, sent, send_sem).wait()
    settled(halo_send, 0)

    @pl.when(has)
    def _():
        settled(halo_send, 1)


def finish(
    comp, ext, weights,
    out_red, out_nir, out_chosen, out_one, out_two, out_three,
    level1, ext1, level2, ext2, one, two, three, comp_sem, sems,
):
    for i, out in enumerate((out_red, out_nir, out_chosen)):
        pltpu.make_async_copy(comp.at[i], out, comp_sem).start()
    pairs = ((one, out_one), (two, out_two), (three, out_three))
    copies = [pltpu.make_async_copy(src, dst, sems.at[i]) for i, (src, dst) in enumerate(pairs)]
    core = lax.axis_index("dates")
    z = lax.axis_index("rows")
    has = jnp.where(core == 0, z > 0, z < lax.axis_size("rows") - 1)
    clear_margins(level1)
    clear_margins(level2)

    def inside(rows, near):
        index = lax.broadcasted_iota(jnp.int32, (rows, 128), 0)
        low = jnp.where(has | (core == 1), 0, near)
        high = jnp.where(has | (core == 0), rows, rows - near)
        return (index >= low) & (index < high)

    def stacked(source, block, start, rows):
        value = TAPS[0] * source[block, pl.ds(start, rows, 2), :]
        for i in range(1, 6):
            value = value + TAPS[i] * source[block, pl.ds(start + i, rows, 2), :]
        return value

    def descend(source, start, rows, keep, near, out, padded, target):
        valid = inside(rows, near)
        blocks = source.shape[0] // 2
        for band in range(2):
            for c in range(blocks):
                value = stacked(source, band * blocks + c, start, rows)
                out[band, :, c * 128 : (c + 1) * 128] = value[keep : keep + out.shape[1]]
                padded[band * rows : (band + 1) * rows, 128 * (c + 1) : 128 * (c + 2)] = jnp.where(valid, value, 0.0)
        spans = blocks * 64 // SPAN
        results = pooled([padded[:, 2 * SPAN * b : 2 * SPAN * b + WINDOW] for b in range(spans)], weights[...])
        for b, result in enumerate(results):
            for band in range(2):
                for i in range(SPAN // 128):
                    target[band * blocks // 2 + b * (SPAN // 128) + i] = result[
                        band * rows : (band + 1) * rows, i * 128 : (i + 1) * 128
                    ]

    descend(ext, 6, 24, 8, 8, one, level1, ext1)
    copies[0].start()
    descend(ext1, 2, 8, 2, 2, two, level2, ext2)
    copies[1].start()
    blocks = ext2.shape[0] // 2
    for band in range(2):
        for c in range(blocks):
            three[band, :, c * 128 : (c + 1) * 128] = stacked(ext2, band * blocks + c, 0, 2)

    copies[2].start()
    for copy in copies:
        copy.wait()
    pltpu.make_async_copy(comp, comp, comp_sem).wait()


def body(red_band, nir_band, cloud_class, date_ordinal):
    dates, strip, cols = red_band.shape
    half = strip // 2
    tiles = half // TILE
    whole = pl.BlockSpec(memory_space=pltpu.VMEM)
    far = pl.BlockSpec(memory_space=pltpu.HBM)
    f32, i32 = jnp.float32, jnp.int32
    arrays = (date_ordinal, red_band, nir_band, cloud_class)
    arrays = [pltpu.with_memory_space_constraint(array, pltpu.HBM) for array in arrays]
    near = pl.pallas_call(
        kernel,
        out_shape=[
            pltpu.VMEM((3, half, cols), i32),
            pltpu.VMEM((cols // 128, 64, 128), f32),
            pltpu.VMEM((WINDOW, SPAN), jnp.bfloat16),
        ],
        in_specs=[far] * 4,
        out_specs=[whole] * 3,
        scratch_shapes=[
            pltpu.SMEM((dates,), i32),
            pltpu.VMEM((2 * tiles, 3, dates, TILE, cols), i32),
            pltpu.VMEM((tiles, 3, TILE, cols), i32),
            pltpu.VMEM((tiles, 3, TILE, cols), i32),
            pltpu.VMEM((tiles, 6, TILE, cols), i32),
            pltpu.VMEM((tiles, 16, cols + 256), f32),
            pltpu.SemaphoreType.DMA((len(pieces_of(tiles, cols)),)),
            pltpu.SemaphoreType.DMA,
            pltpu.SemaphoreType.DMA,
            pltpu.SemaphoreType.DMA((tiles,)),
            pltpu.SemaphoreType.DMA((2,)),
            pltpu.SemaphoreType.DMA((2,)),
        ],
        compiler_params=pltpu.CompilerParams(
            collective_id=0, has_side_effects=True, vmem_limit_bytes=32 * 1024 * 1024
        ),
        name="composite",
    )(*arrays)
    levels = [(2, half >> k, cols >> k) for k in (1, 2, 3)]
    return pl.pallas_call(
        finish,
        out_shape=[jax.ShapeDtypeStruct((half, cols), i32)] * 3 + [jax.ShapeDtypeStruct(shape, f32) for shape in levels],
        in_specs=[whole] * 3,
        out_specs=[far] * 6,
        scratch_shapes=[
            pltpu.VMEM((48, cols // 2 + 256), f32),
            pltpu.VMEM((cols // 256, 24, 128), f32),
            pltpu.VMEM((16, cols // 4 + 256), f32),
            pltpu.VMEM((cols // 512, 8, 128), f32),
        ]
        + [pltpu.VMEM(shape, f32) for shape in levels]
        + [pltpu.SemaphoreType.DMA, pltpu.SemaphoreType.DMA((3,))],
        compiler_params=pltpu.CompilerParams(vmem_limit_bytes=16 * 1024 * 1024),
        name="finish",
    )(*near)


def solution(mesh):
    in_specs = (
        P("dates", ("tiles", "rows"), None),
        P("dates", ("tiles", "rows"), None),
        P("dates", ("tiles", "rows"), None),
        P(("tiles", "dates")),
    )
    out_specs = (
        P(("tiles", "rows", "dates"), None),
        P(("tiles", "rows", "dates"), None),
        P(("tiles", "rows", "dates"), None),
        P(None, ("tiles", "rows", "dates"), None),
        P(None, ("tiles", "rows", "dates"), None),
        P(None, ("tiles", "rows", "dates"), None),
    )
    return jax.shard_map(body, mesh=mesh, in_specs=in_specs, out_specs=out_specs, check_vma=False)
```

```python
import functools

import jax
import jax.numpy as jnp
from jax import lax
from jax.experimental import pallas as pl
from jax.experimental.pallas import tpu as pltpu
from jax.sharding import PartitionSpec as P

MESH = pl.DeviceIdType.MESH
LIMB_BITS = 15
LIMB_MASK = 32767
CLEAR = 1 << 30
FLAG_STEP = 32
SCALE_BAND = 9.313225746154785e-10
TAPS = (0.03125, 0.15625, 0.3125, 0.3125, 0.15625, 0.03125)
TILE = 8
GROUP = 512
SPAN = 256
WINDOW = 2 * SPAN + 256


def split(value):
    return value >> LIMB_BITS, value & LIMB_MASK


def join(high, low):
    return (high << LIMB_BITS) | low


def improve(best, new, bar):
    n1, n0, r1, r0, order = best
    m1, m0, s1, s0, index = new
    low = m0 * r0 - n0 * s0 + ((order - index) >> 31)
    mid = (m1 * r0 + m0 * r1) - (n1 * s0 + n0 * s1) + (low >> LIMB_BITS)
    take = m1 * r1 - n1 * s1 + (mid >> LIMB_BITS) >= bar
    return tuple(jnp.where(take, one, two) for one, two in zip(new, best))


def clear_margins(buffer):
    rows, width = buffer.shape
    buffer[:, 0:128] = jnp.zeros((rows, 128), jnp.float32)
    buffer[:, width - 128 :] = jnp.zeros((rows, 128), jnp.float32)


def pooled(window, weights):
    parts = []
    for block in window:
        head = block.astype(jnp.bfloat16)
        parts += [head, (block - head.astype(jnp.float32)).astype(jnp.bfloat16)]
    rows = window[0].shape[0]
    out = jnp.dot(jnp.concatenate(parts, axis=0), weights, preferred_element_type=jnp.float32)
    return [out[2 * b * rows : (2 * b + 1) * rows] + out[(2 * b + 1) * rows : (2 * b + 2) * rows] for b in range(len(window))]


def place():
    core = lax.axis_index("dates")
    z = lax.axis_index("rows")
    return jnp.where(core == 0, z > 0, z < lax.axis_size("rows") - 1), core


def inside(has, core, rows, near):
    index = lax.broadcasted_iota(jnp.int32, (rows, 128), 0)
    low = jnp.where(has | (core == 1), 0, near)
    high = jnp.where(has | (core == 0), rows, rows - near)
    return (index >= low) & (index < high)


def stacked(source, block, start, rows):
    value = TAPS[0] * source[block, pl.ds(start, rows, 2), :]
    for i in range(1, 6):
        value = value + TAPS[i] * source[block, pl.ds(start + i, rows, 2), :]
    return value


def descend(has, core, weights, source, start, rows, keep, near, out, padded, target):
    valid = inside(has, core, rows, near)
    blocks = source.shape[0] // 2
    for band in range(2):
        for c in range(blocks):
            value = stacked(source, band * blocks + c, start, rows)
            out[band, :, c * 128 : (c + 1) * 128] = value[keep : keep + out.shape[1]]
            padded[band * rows : (band + 1) * rows, 128 * (c + 1) : 128 * (c + 2)] = jnp.where(valid, value, 0.0)
    spans = blocks * 64 // SPAN
    results = pooled([padded[:, 2 * SPAN * b : 2 * SPAN * b + WINDOW] for b in range(spans)], weights[...])
    for b, result in enumerate(results):
        for band in range(2):
            for i in range(SPAN // 128):
                target[band * blocks // 2 + b * (SPAN // 128) + i] = result[
                    band * rows : (band + 1) * rows, i * 128 : (i + 1) * 128
                ]


def pieces_of(tiles, cols):
    half = cols // 2
    first = [(0, 0, GROUP), (0, GROUP, half - GROUP), (0, half, half), (1, 0, half), (1, half, half)]
    return first + [(slot, 0, cols) for slot in range(2, 2 * tiles)]


def kernel(
    ordinal_far, red, nir, cloud,
    comp, one, ext1, weights,
    ordinal, images, sent, got, mine, level, ext, level1,
    in_sem, ordinal_sem, send_sem, recv_sem, halo_send, halo_recv,
):
    dates, strip, cols = red.shape
    half = strip // 2
    tiles = half // TILE
    core = lax.axis_index("dates")
    z = lax.axis_index("rows")
    last = lax.axis_size("rows") - 1
    other = 1 - core
    has = jnp.where(core == 0, z > 0, z < last)
    beyond = jnp.where(core == 0, z - 1, z + 1)
    partner = {"dates": other}
    neighbour = {"rows": beyond, "dates": other}

    def tile_in_half(c, k):
        return jnp.where(c == 0, k, tiles - 1 - k)

    pieces = pieces_of(tiles, cols)

    def load(i):
        slot, start, width = pieces[i]
        owner = other if slot < tiles else core
        row = pl.multiple_of(owner * half + tile_in_half(owner, slot % tiles) * TILE, TILE)
        col = pl.ds(start, width)
        for j, src in enumerate((red, nir, cloud)):
            pltpu.make_async_copy(src.at[:, pl.ds(row, TILE), col], images.at[slot, j, :, :, col], in_sem.at[i]).start()

    def loaded(i):
        slot, start, width = pieces[i]
        there = images.at[slot, :, :, :, pl.ds(start, width)]
        pltpu.make_async_copy(there, there, in_sem.at[i]).wait()

    order_copy = pltpu.make_async_copy(ordinal_far, ordinal, ordinal_sem)
    order_copy.start()
    for i in range(len(pieces)):
        load(i)

    barrier = pltpu.get_barrier_semaphore()
    pl.semaphore_signal(barrier, inc=1, device_id=partner, device_id_type=MESH)

    @pl.when(has)
    def _():
        pl.semaphore_signal(barrier, inc=1, device_id=neighbour, device_id_type=MESH)

    shape = (WINDOW, SPAN)
    tap = lax.broadcasted_iota(jnp.int32, shape, 0) - 2 * lax.broadcasted_iota(jnp.int32, shape, 1) - 126
    factor = jnp.zeros(shape, jnp.float32)
    for i, weight in enumerate(TAPS):
        factor = jnp.where(tap == i, weight, factor)
    weights[...] = factor.astype(jnp.bfloat16)
    for buffer in (*(level.at[k] for k in range(tiles)), level1):
        clear_margins(buffer)
    lanes = ext.shape[0]
    ext[:, 0:8] = jnp.zeros((lanes, 8, 128), jnp.float32)
    ext[:, 56:64] = jnp.zeros((lanes, 8, 128), jnp.float32)

    @pl.when(jnp.logical_not(has))
    def _():
        edge = pl.multiple_of(jnp.where(core == 0, 8, 40), 8)
        ext[:, pl.ds(edge, half)] = jnp.zeros((lanes, half, 128), jnp.float32)

    def best_of(slot, col):
        lowest = images[slot, 2, 0, :, col]
        for d in range(1, dates):
            lowest = jnp.minimum(lowest, images[slot, 2, d, :, col])
        limit = jnp.where(lowest == 0, 0, CLEAR)
        best = None
        for d in range(dates):
            nir_value = jnp.where(images[slot, 2, d, :, col] > limit, 0, images[slot, 1, d, :, col])
            order = jnp.full((TILE, GROUP), ordinal[d], jnp.int32)
            new = (*split(nir_value), *split(images[slot, 0, d, :, col]), order)
            best = new if best is None else improve(best, new, 0)
        return best, lowest == 0

    def exchange(k, col):
        return pltpu.make_async_remote_copy(
            src_ref=sent.at[k, :, :, col],
            dst_ref=got.at[k, :, :, col],
            send_sem=send_sem,
            recv_sem=recv_sem.at[k],
            device_id=partner,
            device_id_type=MESH,
        )

    def columns(start, count):
        return [pl.ds(start + i * GROUP, GROUP) for i in range(count // GROUP)]

    def offer(slot, col):
        (n1, n0, r1, r0, order), is_clear = best_of(slot, col)
        sent[slot, 0, :, col] = join(r1, r0)
        sent[slot, 1, :, col] = join(n1, n0)
        sent[slot, 2, :, col] = order + jnp.where(is_clear, FLAG_STEP, 0)

    order_copy.wait()
    for i, (slot, start, width) in enumerate(pieces):
        if slot < tiles:
            loaded(i)
            for col in columns(start, width):
                offer(slot, col)
            if slot == 0 and start + width == cols:
                pl.semaphore_wait(barrier, jnp.where(has, 2, 1))
                exchange(slot, pl.ds(0, cols)).start()
            if slot > 0:
                exchange(slot, pl.ds(start, width)).start()

    base = len(pieces) - tiles
    for k in range(tiles):
        loaded(base + k)
        for col in columns(0, cols):
            best, is_clear = best_of(tiles + k, col)
            for i, limb in enumerate((*best, jnp.where(is_clear, CLEAR, 0))):
                mine[k, i, :, col] = limb

    def halo(k, side):
        here = tile_in_half(core, k) * TILE
        there = 8 + 32 * (core if side == 0 else other) + here
        return pltpu.make_async_remote_copy(
            src_ref=ext.at[:, pl.ds(pl.multiple_of(24 + here, 8), TILE)],
            dst_ref=ext.at[:, pl.ds(pl.multiple_of(there, 8), TILE)],
            send_sem=halo_send.at[side],
            recv_sem=halo_recv.at[side],
            device_id=partner if side == 0 else neighbour,
            device_id_type=MESH,
        )

    def settle(k):
        row = pl.multiple_of(tile_in_half(core, k) * TILE, TILE)
        for col in columns(0, cols):
            flagged = got[k, 2, :, col]
            is_clear = flagged >= FLAG_STEP
            order = jnp.where(is_clear, flagged - FLAG_STEP, flagged)
            theirs = (*split(got[k, 1, :, col]), *split(got[k, 0, :, col]), order)
            bar = mine[k, 5, :, col] - jnp.where(is_clear, CLEAR, 0)
            n1, n0, r1, r0, order = improve(tuple(mine[k, i, :, col] for i in range(5)), theirs, bar)
            value_red, value_nir = join(r1, r0), join(n1, n0)
            comp[0, pl.ds(row, TILE), col] = value_red
            comp[1, pl.ds(row, TILE), col] = value_nir
            comp[2, pl.ds(row, TILE), col] = order
            inner = pl.ds(col.start + 128, GROUP)
            level[k, 0:8, inner] = value_red.astype(jnp.float32) * SCALE_BAND
            level[k, 8:16, inner] = value_nir.astype(jnp.float32) * SCALE_BAND

    def narrow(k):
        spans = cols // 2 // SPAN
        results = pooled([level[k, :, 2 * SPAN * b : 2 * SPAN * b + WINDOW] for b in range(spans)], weights[...])
        here = pl.ds(pl.multiple_of(24 + tile_in_half(core, k) * TILE, 8), TILE)
        for b, result in enumerate(results):
            for i in range(SPAN // 128):
                piece = slice(i * 128, (i + 1) * 128)
                ext[b * (SPAN // 128) + i, here] = result[0:8, piece]
                ext[lanes // 2 + b * (SPAN // 128) + i, here] = result[8:16, piece]

    for k in range(tiles):
        pltpu.make_async_copy(got.at[k], got.at[k], recv_sem.at[k]).wait()
        settle(k)
        narrow(k)
        halo(k, 0).start()

        @pl.when(has)
        def _():
            halo(k, 1).start()

    def settled(sems, side):
        both = ext.at[:, 8 : 8 + half]
        pltpu.make_async_copy(both, both, sems.at[side]).wait()

    settled(halo_recv, 0)

    @pl.when(has)
    def _():
        settled(halo_recv, 1)

    descend(has, core, weights, ext, 6, 24, 8, 8, one, level1, ext1)
    pltpu.make_async_copy(sent, sent, send_sem).wait()
    settled(halo_send, 0)

    @pl.when(has)
    def _():
        settled(halo_send, 1)


def finish(
    comp, one, ext1, weights,
    out_red, out_nir, out_chosen, out_one, out_two, out_three,
    two, three, level2, ext2, comp_sem, sems,
):
    pairs = ((one, out_one), (two, out_two), (three, out_three))
    copies = [pltpu.make_async_copy(src, dst, sems.at[i]) for i, (src, dst) in enumerate(pairs)]
    for i, out in enumerate((out_red, out_nir, out_chosen)):
        pltpu.make_async_copy(comp.at[i], out, comp_sem).start()
    copies[0].start()
    has, core = place()
    clear_margins(level2)
    descend(has, core, weights, ext1, 2, 8, 2, 2, two, level2, ext2)
    copies[1].start()
    blocks = ext2.shape[0] // 2
    for band in range(2):
        for c in range(blocks):
            three[band, :, c * 128 : (c + 1) * 128] = stacked(ext2, band * blocks + c, 0, 2)
    copies[2].start()
    for copy in copies:
        copy.wait()
    pltpu.make_async_copy(comp, comp, comp_sem).wait()


def body(red_band, nir_band, cloud_class, date_ordinal):
    dates, strip, cols = red_band.shape
    half = strip // 2
    tiles = half // TILE
    whole = pl.BlockSpec(memory_space=pltpu.VMEM)
    far = pl.BlockSpec(memory_space=pltpu.HBM)
    f32, i32 = jnp.float32, jnp.int32
    arrays = (date_ordinal, red_band, nir_band, cloud_class)
    arrays = [pltpu.with_memory_space_constraint(array, pltpu.HBM) for array in arrays]
    levels = [(2, half >> k, cols >> k) for k in (1, 2, 3)]
    near = pl.pallas_call(
        kernel,
        out_shape=[
            pltpu.VMEM((3, half, cols), i32),
            pltpu.VMEM(levels[0], f32),
            pltpu.VMEM((cols // 256, 24, 128), f32),
            pltpu.VMEM((WINDOW, SPAN), jnp.bfloat16),
        ],
        in_specs=[far] * 4,
        out_specs=[whole] * 4,
        scratch_shapes=[
            pltpu.SMEM((dates,), i32),
            pltpu.VMEM((2 * tiles, 3, dates, TILE, cols), i32),
            pltpu.VMEM((tiles, 3, TILE, cols), i32),
            pltpu.VMEM((tiles, 3, TILE, cols), i32),
            pltpu.VMEM((tiles, 6, TILE, cols), i32),
            pltpu.VMEM((tiles, 16, cols + 256), f32),
            pltpu.VMEM((cols // 128, 64, 128), f32),
            pltpu.VMEM((48, cols // 2 + 256), f32),
            pltpu.SemaphoreType.DMA((len(pieces_of(tiles, cols)),)),
            pltpu.SemaphoreType.DMA,
            pltpu.SemaphoreType.DMA,
            pltpu.SemaphoreType.DMA((tiles,)),
            pltpu.SemaphoreType.DMA((2,)),
            pltpu.SemaphoreType.DMA((2,)),
        ],
        compiler_params=pltpu.CompilerParams(
            collective_id=0, has_side_effects=True, vmem_limit_bytes=32 * 1024 * 1024
        ),
        name="composite",
    )(*arrays)
    return pl.pallas_call(
        finish,
        out_shape=[jax.ShapeDtypeStruct((half, cols), i32)] * 3 + [jax.ShapeDtypeStruct(shape, f32) for shape in levels],
        in_specs=[whole] * 4,
        out_specs=[far] * 6,
        scratch_shapes=[
            pltpu.VMEM(levels[1], f32),
            pltpu.VMEM(levels[2], f32),
            pltpu.VMEM((16, cols // 4 + 256), f32),
            pltpu.VMEM((cols // 512, 8, 128), f32),
            pltpu.SemaphoreType.DMA,
            pltpu.SemaphoreType.DMA((3,)),
        ],
        compiler_params=pltpu.CompilerParams(vmem_limit_bytes=16 * 1024 * 1024),
        name="finish",
    )(*near)


def solution(mesh):
    in_specs = (
        P("dates", ("tiles", "rows"), None),
        P("dates", ("tiles", "rows"), None),
        P("dates", ("tiles", "rows"), None),
        P(("tiles", "dates")),
    )
    out_specs = (
        P(("tiles", "rows", "dates"), None),
        P(("tiles", "rows", "dates"), None),
        P(("tiles", "rows", "dates"), None),
        P(None, ("tiles", "rows", "dates"), None),
        P(None, ("tiles", "rows", "dates"), None),
        P(None, ("tiles", "rows", "dates"), None),
    )
    return jax.shard_map(body, mesh=mesh, in_specs=in_specs, out_specs=out_specs, check_vma=False)
```

```python
import functools

import jax
import jax.numpy as jnp
from jax import lax
from jax.experimental import pallas as pl
from jax.experimental.pallas import tpu as pltpu
from jax.sharding import PartitionSpec as P

MESH = pl.DeviceIdType.MESH
LIMB_BITS = 15
LIMB_MASK = 32767
CLEAR = 1 << 30
FLAG_STEP = 32
RADIX_BITS = 4
SCALE_BAND = 9.313225746154785e-10
TAPS = (0.03125, 0.15625, 0.3125, 0.3125, 0.15625, 0.03125)
TILE = 8
GROUP = 256
SPAN = 256
WINDOW = 2 * SPAN + 256


def split(value):
    return value >> LIMB_BITS, value & LIMB_MASK


def join(high, low):
    return (high << LIMB_BITS) | low


def younger(best, new):
    n1, n0, r1, r0, _ = best
    m1, m0, s1, s0, _ = new
    low = n0 * s0 - m0 * r0
    mid = (n1 * s0 + n0 * s1) - (m1 * r0 + m0 * r1) + (low >> LIMB_BITS)
    take = n1 * s1 - m1 * r1 + (mid >> LIMB_BITS) < 0
    return tuple(jnp.where(take, one, two) for one, two in zip(new, best))


def improve(best, new, bar):
    n1, n0, r1, r0, order = best
    m1, m0, s1, s0, index = new
    low = m0 * r0 - n0 * s0 + ((order - index) >> 31)
    mid = (m1 * r0 + m0 * r1) - (n1 * s0 + n0 * s1) + (low >> LIMB_BITS)
    take = m1 * r1 - n1 * s1 + (mid >> LIMB_BITS) >= bar
    return tuple(jnp.where(take, one, two) for one, two in zip(new, best))


def clear_margins(buffer):
    rows, width = buffer.shape
    buffer[:, 0:128] = jnp.zeros((rows, 128), jnp.float32)
    buffer[:, width - 128 :] = jnp.zeros((rows, 128), jnp.float32)


def pooled(window, weights):
    parts = []
    for block in window:
        head = block.astype(jnp.bfloat16)
        parts += [head, (block - head.astype(jnp.float32)).astype(jnp.bfloat16)]
    rows = window[0].shape[0]
    out = jnp.dot(jnp.concatenate(parts, axis=0), weights, preferred_element_type=jnp.float32)
    return [out[2 * b * rows : (2 * b + 1) * rows] + out[(2 * b + 1) * rows : (2 * b + 2) * rows] for b in range(len(window))]


def place():
    core = lax.axis_index("dates")
    z = lax.axis_index("rows")
    return jnp.where(core == 0, z > 0, z < lax.axis_size("rows") - 1), core


def inside(has, core, rows, near):
    index = lax.broadcasted_iota(jnp.int32, (rows, 128), 0)
    low = jnp.where(has | (core == 1), 0, near)
    high = jnp.where(has | (core == 0), rows, rows - near)
    return (index >= low) & (index < high)


def stacked(source, block, start, rows):
    value = TAPS[0] * source[block, pl.ds(start, rows, 2), :]
    for i in range(1, 6):
        value = value + TAPS[i] * source[block, pl.ds(start + i, rows, 2), :]
    return value


def descend(has, core, weights, source, start, rows, keep, near, out, padded, target):
    valid = inside(has, core, rows, near)
    blocks = source.shape[0] // 2
    for band in range(2):
        for c in range(blocks):
            value = stacked(source, band * blocks + c, start, rows)
            out[band, :, c * 128 : (c + 1) * 128] = value[keep : keep + out.shape[1]]
            padded[band * rows : (band + 1) * rows, 128 * (c + 1) : 128 * (c + 2)] = jnp.where(valid, value, 0.0)
    spans = blocks * 64 // SPAN
    results = pooled([padded[:, 2 * SPAN * b : 2 * SPAN * b + WINDOW] for b in range(spans)], weights[...])
    for b, result in enumerate(results):
        for band in range(2):
            for i in range(SPAN // 128):
                target[band * blocks // 2 + b * (SPAN // 128) + i] = result[
                    band * rows : (band + 1) * rows, i * 128 : (i + 1) * 128
                ]


def network(count):
    pairs, p = [], 1
    while p < count:
        k = p
        while k >= 1:
            for j in range(k % p, count - k, 2 * k):
                for i in range(j, j + min(k, count - j - k)):
                    if i // (2 * p) == (i + k) // (2 * p):
                        pairs.append((i, i + k))
            k //= 2
        p *= 2
    return pairs


def pieces_of(tiles, cols):
    widths = [4 * GROUP, 4 * GROUP, 4 * GROUP] + [cols] * (2 * tiles - 3)
    return [(slot, col, width) for slot, width in enumerate(widths) for col in range(0, cols, width)]


def kernel(
    ordinal_far, red, nir, cloud,
    comp, one, ext1, weights,
    ordinal, ranked, sent, got, mine, level, ext, level1,
    in_sem, ordinal_sem, send_sem, recv_sem, halo_send, halo_recv, *images
):
    dates, strip, cols = red.shape
    half = strip // 2
    tiles = half // TILE
    core = lax.axis_index("dates")
    z = lax.axis_index("rows")
    last = lax.axis_size("rows") - 1
    other = 1 - core
    has = jnp.where(core == 0, z > 0, z < last)
    beyond = jnp.where(core == 0, z - 1, z + 1)
    partner = {"dates": other}
    neighbour = {"rows": beyond, "dates": other}

    def tile_in_half(c, k):
        return jnp.where(c == 0, k, tiles - 1 - k)

    pieces = pieces_of(tiles, cols)

    def load(i):
        slot, start, width = pieces[i]
        owner = other if slot < tiles else core
        row = pl.multiple_of(owner * half + tile_in_half(owner, slot % tiles) * TILE, TILE)
        col = pl.ds(start, width)
        for j, src in enumerate((red, nir, cloud)):
            pltpu.make_async_copy(src.at[:, pl.ds(row, TILE), col], images[i].at[j], in_sem.at[i]).start()

    def loaded(i):
        pltpu.make_async_copy(images[i], images[i], in_sem.at[i]).wait()

    order_copy = pltpu.make_async_copy(ordinal_far, ordinal, ordinal_sem)
    order_copy.start()
    for i in range(len(pieces)):
        load(i)

    barrier = pltpu.get_barrier_semaphore()
    pl.semaphore_signal(barrier, inc=1, device_id=partner, device_id_type=MESH)

    @pl.when(has)
    def _():
        pl.semaphore_signal(barrier, inc=1, device_id=neighbour, device_id_type=MESH)

    shape = (WINDOW, SPAN)
    tap = lax.broadcasted_iota(jnp.int32, shape, 0) - 2 * lax.broadcasted_iota(jnp.int32, shape, 1) - 126
    factor = jnp.zeros(shape, jnp.float32)
    for i, weight in enumerate(TAPS):
        factor = jnp.where(tap == i, weight, factor)
    weights[...] = factor.astype(jnp.bfloat16)
    for buffer in (*(level.at[k] for k in range(tiles)), level1):
        clear_margins(buffer)
    lanes = ext.shape[0]
    ext[:, 0:8] = jnp.zeros((lanes, 8, 128), jnp.float32)
    ext[:, 56:64] = jnp.zeros((lanes, 8, 128), jnp.float32)

    @pl.when(jnp.logical_not(has))
    def _():
        edge = pl.multiple_of(jnp.where(core == 0, 8, 40), 8)
        ext[:, pl.ds(edge, half)] = jnp.zeros((lanes, half, 128), jnp.float32)

    def best_of(image, col):
        product = image[2, 0, :, col]
        for d in range(1, dates):
            product = product * image[2, d, :, col]
        limit = jnp.where(product == 0, 0, CLEAR)
        best = None
        for d in range(dates):
            at = ranked[0, d]
            nir_value = jnp.where(image[2, at, :, col] > limit, 0, image[1, at, :, col])
            order = jnp.full((TILE, GROUP), ranked[1, d], jnp.int32)
            new = (*split(nir_value), *split(image[0, at, :, col]), order)
            best = new if best is None else younger(best, new)
        return best, product == 0

    def exchange(k, col):
        return pltpu.make_async_remote_copy(
            src_ref=sent.at[k, :, :, col],
            dst_ref=got.at[k, :, :, col],
            send_sem=send_sem,
            recv_sem=recv_sem.at[k],
            device_id=partner,
            device_id_type=MESH,
        )

    def columns(start, count):
        return [pl.ds(start + i * GROUP, GROUP) for i in range(count // GROUP)]

    def offer(i, slot, col, inner):
        (n1, n0, r1, r0, order), is_clear = best_of(images[i], inner)
        sent[slot, 0, :, col] = join(r1, r0)
        sent[slot, 1, :, col] = join(n1, n0)
        sent[slot, 2, :, col] = order + jnp.where(is_clear, FLAG_STEP, 0)

    order_copy.wait()
    keys = [(ordinal[d] << RADIX_BITS) + d for d in range(dates)]
    for i, j in network(dates):
        keys[i], keys[j] = jnp.minimum(keys[i], keys[j]), jnp.maximum(keys[i], keys[j])
    for d, key in enumerate(keys):
        ranked[0, d] = key & ((1 << RADIX_BITS) - 1)
        ranked[1, d] = key >> RADIX_BITS
    for i, (slot, start, width) in enumerate(pieces):
        if slot < tiles:
            loaded(i)
            for col, inner in zip(columns(start, width), columns(0, width)):
                offer(i, slot, col, inner)
            if slot == 0 and start + width == cols:
                pl.semaphore_wait(barrier, jnp.where(has, 2, 1))
                exchange(slot, pl.ds(0, cols)).start()
            if slot > 0:
                exchange(slot, pl.ds(start, width)).start()

    for i, (slot, start, width) in enumerate(pieces):
        if slot >= tiles:
            loaded(i)
            for col, inner in zip(columns(start, width), columns(0, width)):
                best, is_clear = best_of(images[i], inner)
                for j, limb in enumerate((*best, jnp.where(is_clear, CLEAR, 0))):
                    mine[slot - tiles, j, :, col] = limb

    def halo(k, side):
        here = tile_in_half(core, k) * TILE
        there = 8 + 32 * (core if side == 0 else other) + here
        return pltpu.make_async_remote_copy(
            src_ref=ext.at[:, pl.ds(pl.multiple_of(24 + here, 8), TILE)],
            dst_ref=ext.at[:, pl.ds(pl.multiple_of(there, 8), TILE)],
            send_sem=halo_send.at[side],
            recv_sem=halo_recv.at[side],
            device_id=partner if side == 0 else neighbour,
            device_id_type=MESH,
        )

    def settle(k):
        row = pl.multiple_of(tile_in_half(core, k) * TILE, TILE)
        for col in columns(0, cols):
            flagged = got[k, 2, :, col]
            is_clear = flagged >= FLAG_STEP
            order = jnp.where(is_clear, flagged - FLAG_STEP, flagged)
            theirs = (*split(got[k, 1, :, col]), *split(got[k, 0, :, col]), order)
            bar = mine[k, 5, :, col] - jnp.where(is_clear, CLEAR, 0)
            n1, n0, r1, r0, order = improve(tuple(mine[k, i, :, col] for i in range(5)), theirs, bar)
            value_red, value_nir = join(r1, r0), join(n1, n0)
            comp[0, pl.ds(row, TILE), col] = value_red
            comp[1, pl.ds(row, TILE), col] = value_nir
            comp[2, pl.ds(row, TILE), col] = order
            inner = pl.ds(col.start + 128, GROUP)
            level[k, 0:8, inner] = value_red.astype(jnp.float32) * SCALE_BAND
            level[k, 8:16, inner] = value_nir.astype(jnp.float32) * SCALE_BAND

    def narrow(k):
        spans = cols // 2 // SPAN
        results = pooled([level[k, :, 2 * SPAN * b : 2 * SPAN * b + WINDOW] for b in range(spans)], weights[...])
        here = pl.ds(pl.multiple_of(24 + tile_in_half(core, k) * TILE, 8), TILE)
        for b, result in enumerate(results):
            for i in range(SPAN // 128):
                piece = slice(i * 128, (i + 1) * 128)
                ext[b * (SPAN // 128) + i, here] = result[0:8, piece]
                ext[lanes // 2 + b * (SPAN // 128) + i, here] = result[8:16, piece]

    for k in range(tiles):
        pltpu.make_async_copy(got.at[k], got.at[k], recv_sem.at[k]).wait()
        settle(k)
        narrow(k)
        halo(k, 0).start()

        @pl.when(has)
        def _():
            halo(k, 1).start()

    def settled(sems, side):
        both = ext.at[:, 8 : 8 + half]
        pltpu.make_async_copy(both, both, sems.at[side]).wait()

    settled(halo_recv, 0)

    @pl.when(has)
    def _():
        settled(halo_recv, 1)

    descend(has, core, weights, ext, 6, 24, 8, 8, one, level1, ext1)
    pltpu.make_async_copy(sent, sent, send_sem).wait()
    settled(halo_send, 0)

    @pl.when(has)
    def _():
        settled(halo_send, 1)


def finish(
    comp, one, ext1, weights,
    out_red, out_nir, out_chosen, out_one, out_two, out_three,
    two, three, level2, ext2, comp_sem, sems,
):
    pairs = ((one, out_one), (two, out_two), (three, out_three))
    copies = [pltpu.make_async_copy(src, dst, sems.at[i]) for i, (src, dst) in enumerate(pairs)]
    for i, out in enumerate((out_red, out_nir, out_chosen)):
        pltpu.make_async_copy(comp.at[i], out, comp_sem).start()
    copies[0].start()
    has, core = place()
    clear_margins(level2)
    descend(has, core, weights, ext1, 2, 8, 2, 2, two, level2, ext2)
    copies[1].start()
    blocks = ext2.shape[0] // 2
    for band in range(2):
        for c in range(blocks):
            three[band, :, c * 128 : (c + 1) * 128] = stacked(ext2, band * blocks + c, 0, 2)
    copies[2].start()
    for copy in copies:
        copy.wait()
    pltpu.make_async_copy(comp, comp, comp_sem).wait()


def body(red_band, nir_band, cloud_class, date_ordinal):
    dates, strip, cols = red_band.shape
    half = strip // 2
    tiles = half // TILE
    whole = pl.BlockSpec(memory_space=pltpu.VMEM)
    far = pl.BlockSpec(memory_space=pltpu.HBM)
    f32, i32 = jnp.float32, jnp.int32
    arrays = (date_ordinal, red_band, nir_band, cloud_class)
    arrays = [pltpu.with_memory_space_constraint(array, pltpu.HBM) for array in arrays]
    levels = [(2, half >> k, cols >> k) for k in (1, 2, 3)]
    near = pl.pallas_call(
        kernel,
        out_shape=[
            pltpu.VMEM((3, half, cols), i32),
            pltpu.VMEM(levels[0], f32),
            pltpu.VMEM((cols // 256, 24, 128), f32),
            pltpu.VMEM((WINDOW, SPAN), jnp.bfloat16),
        ],
        in_specs=[far] * 4,
        out_specs=[whole] * 4,
        scratch_shapes=[
            pltpu.SMEM((dates,), i32),
            pltpu.SMEM((2, dates), i32),
            pltpu.VMEM((tiles, 3, TILE, cols), i32),
            pltpu.VMEM((tiles, 3, TILE, cols), i32),
            pltpu.VMEM((tiles, 6, TILE, cols), i32),
            pltpu.VMEM((tiles, 16, cols + 256), f32),
            pltpu.VMEM((cols // 128, 64, 128), f32),
            pltpu.VMEM((48, cols // 2 + 256), f32),
            pltpu.SemaphoreType.DMA((len(pieces_of(tiles, cols)),)),
            pltpu.SemaphoreType.DMA,
            pltpu.SemaphoreType.DMA,
            pltpu.SemaphoreType.DMA((tiles,)),
            pltpu.SemaphoreType.DMA((2,)),
            pltpu.SemaphoreType.DMA((2,)),
        ]
        + [pltpu.VMEM((3, dates, TILE, width), i32) for _, _, width in pieces_of(tiles, cols)],
        compiler_params=pltpu.CompilerParams(
            collective_id=0, has_side_effects=True, vmem_limit_bytes=32 * 1024 * 1024
        ),
        name="composite",
    )(*arrays)
    return pl.pallas_call(
        finish,
        out_shape=[jax.ShapeDtypeStruct((half, cols), i32)] * 3 + [jax.ShapeDtypeStruct(shape, f32) for shape in levels],
        in_specs=[whole] * 4,
        out_specs=[far] * 6,
        scratch_shapes=[
            pltpu.VMEM(levels[1], f32),
            pltpu.VMEM(levels[2], f32),
            pltpu.VMEM((16, cols // 4 + 256), f32),
            pltpu.VMEM((cols // 512, 8, 128), f32),
            pltpu.SemaphoreType.DMA,
            pltpu.SemaphoreType.DMA((3,)),
        ],
        compiler_params=pltpu.CompilerParams(vmem_limit_bytes=16 * 1024 * 1024),
        name="finish",
    )(*near)


def solution(mesh):
    in_specs = (
        P("dates", ("tiles", "rows"), None),
        P("dates", ("tiles", "rows"), None),
        P("dates", ("tiles", "rows"), None),
        P(("tiles", "dates")),
    )
    out_specs = (
        P(("tiles", "rows", "dates"), None),
        P(("tiles", "rows", "dates"), None),
        P(("tiles", "rows", "dates"), None),
        P(None, ("tiles", "rows", "dates"), None),
        P(None, ("tiles", "rows", "dates"), None),
        P(None, ("tiles", "rows", "dates"), None),
    )
    return jax.shard_map(body, mesh=mesh, in_specs=in_specs, out_specs=out_specs, check_vma=False)
```

```python
import functools

import jax
import jax.numpy as jnp
from jax import lax
from jax.experimental import pallas as pl
from jax.experimental.pallas import tpu as pltpu
from jax.sharding import PartitionSpec as P

MESH = pl.DeviceIdType.MESH
LIMB_BITS = 15
LIMB_MASK = 32767
CLEAR = 1 << 30
FLAG_STEP = 32
RADIX_BITS = 4
SCALE_BAND = 9.313225746154785e-10
TAPS = (0.03125, 0.15625, 0.3125, 0.3125, 0.15625, 0.03125)
TILE = 8
GROUP = 256
SPAN = 256
WINDOW = 2 * SPAN + 256


def split(value):
    return value >> LIMB_BITS, value & LIMB_MASK


def join(high, low):
    return (high << LIMB_BITS) | low


def younger(best, new):
    n1, n0, r1, r0, _ = best
    m1, m0, s1, s0, _ = new
    low = n0 * s0 - m0 * r0
    mid = (n1 * s0 + n0 * s1) - (m1 * r0 + m0 * r1) + (low >> LIMB_BITS)
    take = n1 * s1 - m1 * r1 + (mid >> LIMB_BITS) < 0
    return tuple(jnp.where(take, one, two) for one, two in zip(new, best))


def improve(best, new, bar):
    n1, n0, r1, r0, order = best
    m1, m0, s1, s0, index = new
    low = m0 * r0 - n0 * s0 + ((order - index) >> 31)
    mid = (m1 * r0 + m0 * r1) - (n1 * s0 + n0 * s1) + (low >> LIMB_BITS)
    take = m1 * r1 - n1 * s1 + (mid >> LIMB_BITS) >= bar
    return tuple(jnp.where(take, one, two) for one, two in zip(new, best))


def clear_margins(buffer):
    rows, width = buffer.shape
    buffer[:, 0:128] = jnp.zeros((rows, 128), jnp.float32)
    buffer[:, width - 128 :] = jnp.zeros((rows, 128), jnp.float32)


def pooled(window, weights):
    parts = []
    for block in window:
        head = block.astype(jnp.bfloat16)
        parts += [head, (block - head.astype(jnp.float32)).astype(jnp.bfloat16)]
    rows = window[0].shape[0]
    out = jnp.dot(jnp.concatenate(parts, axis=0), weights, preferred_element_type=jnp.float32)
    return [out[2 * b * rows : (2 * b + 1) * rows] + out[(2 * b + 1) * rows : (2 * b + 2) * rows] for b in range(len(window))]


def place():
    core = lax.axis_index("dates")
    z = lax.axis_index("rows")
    return jnp.where(core == 0, z > 0, z < lax.axis_size("rows") - 1), core


def inside(has, core, rows, near):
    index = lax.broadcasted_iota(jnp.int32, (rows, 128), 0)
    low = jnp.where(has | (core == 1), 0, near)
    high = jnp.where(has | (core == 0), rows, rows - near)
    return (index >= low) & (index < high)


def stacked(source, block, start, rows):
    value = TAPS[0] * source[block, pl.ds(start, rows, 2), :]
    for i in range(1, 6):
        value = value + TAPS[i] * source[block, pl.ds(start + i, rows, 2), :]
    return value


def descend(has, core, weights, source, start, rows, keep, near, out, padded, target):
    valid = inside(has, core, rows, near)
    blocks = source.shape[0] // 2
    for band in range(2):
        for c in range(blocks):
            value = stacked(source, band * blocks + c, start, rows)
            out[band, :, c * 128 : (c + 1) * 128] = value[keep : keep + out.shape[1]]
            padded[band * rows : (band + 1) * rows, 128 * (c + 1) : 128 * (c + 2)] = jnp.where(valid, value, 0.0)
    spans = blocks * 64 // SPAN
    results = pooled([padded[:, 2 * SPAN * b : 2 * SPAN * b + WINDOW] for b in range(spans)], weights[...])
    for b, result in enumerate(results):
        for band in range(2):
            for i in range(SPAN // 128):
                target[band * blocks // 2 + b * (SPAN // 128) + i, 0:rows] = result[
                    band * rows : (band + 1) * rows, i * 128 : (i + 1) * 128
                ]


def network(count):
    pairs, p = [], 1
    while p < count:
        k = p
        while k >= 1:
            for j in range(k % p, count - k, 2 * k):
                for i in range(j, j + min(k, count - j - k)):
                    if i // (2 * p) == (i + k) // (2 * p):
                        pairs.append((i, i + k))
            k //= 2
        p *= 2
    return pairs


def pieces_of(tiles, cols):
    widths = [4 * GROUP, 4 * GROUP, 4 * GROUP] + [cols] * (2 * tiles - 3)
    return [(slot, col, width) for slot, width in enumerate(widths) for col in range(0, cols, width)]


def kernel(
    ordinal_far, red, nir, cloud,
    comp, one, ext1, weights,
    ordinal, ranked, sent, got, mine, level, ext, level1,
    in_sem, ordinal_sem, send_sem, recv_sem, halo_send, halo_recv, *images
):
    dates, strip, cols = red.shape
    half = strip // 2
    tiles = half // TILE
    core = lax.axis_index("dates")
    z = lax.axis_index("rows")
    last = lax.axis_size("rows") - 1
    other = 1 - core
    has = jnp.where(core == 0, z > 0, z < last)
    beyond = jnp.where(core == 0, z - 1, z + 1)
    partner = {"dates": other}
    neighbour = {"rows": beyond, "dates": other}

    def tile_in_half(c, k):
        return jnp.where(c == 0, k, tiles - 1 - k)

    pieces = pieces_of(tiles, cols)

    def load(i):
        slot, start, width = pieces[i]
        owner = other if slot < tiles else core
        row = pl.multiple_of(owner * half + tile_in_half(owner, slot % tiles) * TILE, TILE)
        col = pl.ds(start, width)
        for j, src in enumerate((red, nir, cloud)):
            pltpu.make_async_copy(src.at[:, pl.ds(row, TILE), col], images[i].at[j], in_sem.at[i]).start()

    def loaded(i):
        pltpu.make_async_copy(images[i], images[i], in_sem.at[i]).wait()

    order_copy = pltpu.make_async_copy(ordinal_far, ordinal, ordinal_sem)
    order_copy.start()
    for i in range(len(pieces)):
        load(i)

    barrier = pltpu.get_barrier_semaphore()
    pl.semaphore_signal(barrier, inc=1, device_id=partner, device_id_type=MESH)

    @pl.when(has)
    def _():
        pl.semaphore_signal(barrier, inc=1, device_id=neighbour, device_id_type=MESH)

    shape = (WINDOW, SPAN)
    tap = lax.broadcasted_iota(jnp.int32, shape, 0) - 2 * lax.broadcasted_iota(jnp.int32, shape, 1) - 126
    factor = jnp.zeros(shape, jnp.float32)
    for i, weight in enumerate(TAPS):
        factor = jnp.where(tap == i, weight, factor)
    weights[...] = factor.astype(jnp.bfloat16)
    for buffer in (*(level.at[k] for k in range(tiles + 1)), level1):
        clear_margins(buffer)
    lanes = ext.shape[0]
    ext[:, 0:8] = jnp.zeros((lanes, 8, 128), jnp.float32)
    ext[:, 56:64] = jnp.zeros((lanes, 8, 128), jnp.float32)

    @pl.when(jnp.logical_not(has))
    def _():
        edge = pl.multiple_of(jnp.where(core == 0, 8, 40), 8)
        ext[:, pl.ds(edge, half)] = jnp.zeros((lanes, half, 128), jnp.float32)

    def best_of(image, col):
        product = image[2, 0, :, col]
        for d in range(1, dates):
            product = product * image[2, d, :, col]
        limit = jnp.where(product == 0, 0, CLEAR)
        best = None
        for d in range(dates):
            at = ranked[0, d]
            nir_value = jnp.where(image[2, at, :, col] > limit, 0, image[1, at, :, col])
            order = jnp.full((TILE, GROUP), ranked[1, d], jnp.int32)
            new = (*split(nir_value), *split(image[0, at, :, col]), order)
            best = new if best is None else younger(best, new)
        return best, product == 0

    def exchange(k, col):
        return pltpu.make_async_remote_copy(
            src_ref=sent.at[k, :, :, col],
            dst_ref=got.at[k, :, :, col],
            send_sem=send_sem,
            recv_sem=recv_sem.at[k],
            device_id=partner,
            device_id_type=MESH,
        )

    def columns(start, count):
        return [pl.ds(start + i * GROUP, GROUP) for i in range(count // GROUP)]

    def offer(best, is_clear, k, col):
        n1, n0, r1, r0, order = best
        sent[k, 0, :, col] = join(r1, r0)
        sent[k, 1, :, col] = join(n1, n0)
        sent[k, 2, :, col] = order + jnp.where(is_clear, FLAG_STEP, 0)

    order_copy.wait()
    keys = [(ordinal[d] << RADIX_BITS) + d for d in range(dates)]
    for i, j in network(dates):
        keys[i], keys[j] = jnp.minimum(keys[i], keys[j]), jnp.maximum(keys[i], keys[j])
    for d, key in enumerate(keys):
        ranked[0, d] = key & ((1 << RADIX_BITS) - 1)
        ranked[1, d] = key >> RADIX_BITS
    for i, (slot, start, width) in enumerate(pieces):
        if slot < tiles:
            loaded(i)
            for col, inner in zip(columns(start, width), columns(0, width)):
                offer(*best_of(images[i], inner), slot, col)
            if slot == 0 and start + width == cols:
                pl.semaphore_wait(barrier, jnp.where(has, 2, 1))
                exchange(slot, pl.ds(0, cols)).start()
            if slot > 0:
                exchange(slot, pl.ds(start, width)).start()

    for i, (slot, start, width) in enumerate(pieces):
        if slot >= tiles:
            loaded(i)
            for col, inner in zip(columns(start, width), columns(0, width)):
                best, is_clear = best_of(images[i], inner)
                for j, limb in enumerate((*best, jnp.where(is_clear, CLEAR, 0))):
                    mine[slot - tiles, j, :, col] = limb
                if slot == 2 * tiles - 1:
                    offer(best, is_clear, tiles, col)
    exchange(tiles, pl.ds(0, cols)).start()

    def halo(k, side):
        here = tile_in_half(core, k) * TILE
        there = 8 + 32 * (core if side == 0 else other) + here
        return pltpu.make_async_remote_copy(
            src_ref=ext.at[:, pl.ds(pl.multiple_of(24 + here, 8), TILE)],
            dst_ref=ext.at[:, pl.ds(pl.multiple_of(there, 8), TILE)],
            send_sem=halo_send.at[side],
            recv_sem=halo_recv.at[side],
            device_id=partner if side == 0 else neighbour,
            device_id_type=MESH,
        )

    def unpack(packed, k, col):
        flagged = packed[k, 2, :, col]
        is_clear = flagged >= FLAG_STEP
        order = jnp.where(is_clear, flagged - FLAG_STEP, flagged)
        return (*split(packed[k, 1, :, col]), *split(packed[k, 0, :, col]), order), jnp.where(is_clear, CLEAR, 0)

    def fill(k, col, value_red, value_nir):
        inner = pl.ds(col.start + 128, GROUP)
        level[k, 0:8, inner] = value_red.astype(jnp.float32) * SCALE_BAND
        level[k, 8:16, inner] = value_nir.astype(jnp.float32) * SCALE_BAND

    def settle(k):
        row = pl.multiple_of(tile_in_half(core, k) * TILE, TILE)
        for col in columns(0, cols):
            theirs, fresh = unpack(got, k, col)
            bar = mine[k, 5, :, col] - fresh
            n1, n0, r1, r0, order = improve(tuple(mine[k, i, :, col] for i in range(5)), theirs, bar)
            value_red, value_nir = join(r1, r0), join(n1, n0)
            comp[0, pl.ds(row, TILE), col] = value_red
            comp[1, pl.ds(row, TILE), col] = value_nir
            comp[2, pl.ds(row, TILE), col] = order
            fill(k, col, value_red, value_nir)

    def settle_beside():
        for col in columns(0, cols):
            ours, clear = unpack(sent, tiles - 1, col)
            theirs, fresh = unpack(got, tiles, col)
            n1, n0, r1, r0, _ = improve(ours, theirs, clear - fresh)
            fill(tiles, col, join(r1, r0), join(n1, n0))

    def narrow(k, row):
        spans = cols // 2 // SPAN
        results = pooled([level[k, :, 2 * SPAN * b : 2 * SPAN * b + WINDOW] for b in range(spans)], weights[...])
        here = pl.ds(pl.multiple_of(row, 8), TILE)
        for b, result in enumerate(results):
            for i in range(SPAN // 128):
                piece = slice(i * 128, (i + 1) * 128)
                ext[b * (SPAN // 128) + i, here] = result[0:8, piece]
                ext[lanes // 2 + b * (SPAN // 128) + i, here] = result[8:16, piece]

    for k in range(tiles):
        pltpu.make_async_copy(got.at[k], got.at[k], recv_sem.at[k]).wait()
        settle(k)
        narrow(k, 24 + tile_in_half(core, k) * TILE)
        if k < tiles - 1:
            halo(k, 0).start()

        @pl.when(has)
        def _():
            halo(k, 1).start()

    pltpu.make_async_copy(got.at[tiles], got.at[tiles], recv_sem.at[tiles]).wait()
    settle_beside()
    narrow(tiles, 8 + 32 * other + tile_in_half(other, tiles - 1) * TILE)

    def settled(sems, side):
        rows = ext.at[:, 8 : 8 + (half if side == 1 else half - TILE)]
        pltpu.make_async_copy(rows, rows, sems.at[side]).wait()

    settled(halo_recv, 0)

    @pl.when(has)
    def _():
        settled(halo_recv, 1)

    descend(has, core, weights, ext, 6, 24, 8, 8, one, level1, ext1)
    pltpu.make_async_copy(sent, sent, send_sem).wait()
    settled(halo_send, 0)

    @pl.when(has)
    def _():
        settled(halo_send, 1)


def finish(
    comp, one, ext1, weights,
    out_red, out_nir, out_chosen, out_one, out_two, out_three,
    two, three, level2, ext2, comp_sem, sems,
):
    pairs = ((one, out_one), (two, out_two), (three, out_three))
    copies = [pltpu.make_async_copy(src, dst, sems.at[i]) for i, (src, dst) in enumerate(pairs)]
    for i, out in enumerate((out_red, out_nir, out_chosen)):
        pltpu.make_async_copy(comp.at[i], out, comp_sem).start()
    copies[0].start()
    has, core = place()
    clear_margins(level2)
    descend(has, core, weights, ext1, 2, 8, 2, 2, two, level2, ext2)
    copies[1].start()
    blocks = ext2.shape[0] // 2
    for band in range(2):
        for c in range(blocks):
            three[band, :, c * 128 : (c + 1) * 128] = stacked(ext2, band * blocks + c, 0, 2)
    copies[2].start()
    for copy in copies:
        copy.wait()
    pltpu.make_async_copy(comp, comp, comp_sem).wait()


def body(red_band, nir_band, cloud_class, date_ordinal):
    dates, strip, cols = red_band.shape
    half = strip // 2
    tiles = half // TILE
    whole = pl.BlockSpec(memory_space=pltpu.VMEM)
    far = pl.BlockSpec(memory_space=pltpu.HBM)
    f32, i32 = jnp.float32, jnp.int32
    arrays = (date_ordinal, red_band, nir_band, cloud_class)
    arrays = [pltpu.with_memory_space_constraint(array, pltpu.HBM) for array in arrays]
    levels = [(2, half >> k, cols >> k) for k in (1, 2, 3)]
    near = pl.pallas_call(
        kernel,
        out_shape=[
            pltpu.VMEM((3, half, cols), i32),
            pltpu.VMEM(levels[0], f32),
            pltpu.VMEM((cols // 256, 24, 128), f32),
            pltpu.VMEM((WINDOW, SPAN), jnp.bfloat16),
        ],
        in_specs=[far] * 4,
        out_specs=[whole] * 4,
        scratch_shapes=[
            pltpu.SMEM((dates,), i32),
            pltpu.SMEM((2, dates), i32),
            pltpu.VMEM((tiles + 1, 3, TILE, cols), i32),
            pltpu.VMEM((tiles + 1, 3, TILE, cols), i32),
            pltpu.VMEM((tiles, 6, TILE, cols), i32),
            pltpu.VMEM((tiles + 1, 16, cols + 256), f32),
            pltpu.VMEM((cols // 128, 64, 128), f32),
            pltpu.VMEM((48, cols // 2 + 256), f32),
            pltpu.SemaphoreType.DMA((len(pieces_of(tiles, cols)),)),
            pltpu.SemaphoreType.DMA,
            pltpu.SemaphoreType.DMA,
            pltpu.SemaphoreType.DMA((tiles + 1,)),
            pltpu.SemaphoreType.DMA((2,)),
            pltpu.SemaphoreType.DMA((2,)),
        ]
        + [pltpu.VMEM((3, dates, TILE, width), i32) for _, _, width in pieces_of(tiles, cols)],
        compiler_params=pltpu.CompilerParams(
            collective_id=0, has_side_effects=True, vmem_limit_bytes=32 * 1024 * 1024
        ),
        name="composite",
    )(*arrays)
    return pl.pallas_call(
        finish,
        out_shape=[jax.ShapeDtypeStruct((half, cols), i32)] * 3 + [jax.ShapeDtypeStruct(shape, f32) for shape in levels],
        in_specs=[whole] * 4,
        out_specs=[far] * 6,
        scratch_shapes=[
            pltpu.VMEM(levels[1], f32),
            pltpu.VMEM(levels[2], f32),
            pltpu.VMEM((16, cols // 4 + 256), f32),
            pltpu.VMEM((cols // 512, 24, 128), f32),
            pltpu.SemaphoreType.DMA,
            pltpu.SemaphoreType.DMA((3,)),
        ],
        compiler_params=pltpu.CompilerParams(vmem_limit_bytes=16 * 1024 * 1024),
        name="finish",
    )(*near)


def solution(mesh):
    in_specs = (
        P("dates", ("tiles", "rows"), None),
        P("dates", ("tiles", "rows"), None),
        P("dates", ("tiles", "rows"), None),
        P(("tiles", "dates")),
    )
    out_specs = (
        P(("tiles", "rows", "dates"), None),
        P(("tiles", "rows", "dates"), None),
        P(("tiles", "rows", "dates"), None),
        P(None, ("tiles", "rows", "dates"), None),
        P(None, ("tiles", "rows", "dates"), None),
        P(None, ("tiles", "rows", "dates"), None),
    )
    return jax.shard_map(body, mesh=mesh, in_specs=in_specs, out_specs=out_specs, check_vma=False)
```

```python
import functools

import jax
import jax.numpy as jnp
from jax import lax
from jax.experimental import pallas as pl
from jax.experimental.pallas import tpu as pltpu
from jax.sharding import PartitionSpec as P

MESH = pl.DeviceIdType.MESH
LIMB_BITS = 15
LIMB_MASK = 32767
CLEAR = 1 << 30
FLAG_STEP = 32
RADIX_BITS = 4
SCALE_BAND = 9.313225746154785e-10
TAPS = (0.03125, 0.15625, 0.3125, 0.3125, 0.15625, 0.03125)
TILE = 8
REACH = 6
GROUP = 256
SPAN = 256
WINDOW = 2 * SPAN + 256


def split(value):
    return value >> LIMB_BITS, value & LIMB_MASK


def join(high, low):
    return (high << LIMB_BITS) | low


def younger(best, new):
    n1, n0, r1, r0, _ = best
    m1, m0, s1, s0, _ = new
    low = n0 * s0 - m0 * r0
    mid = (n1 * s0 + n0 * s1) - (m1 * r0 + m0 * r1) + (low >> LIMB_BITS)
    take = n1 * s1 - m1 * r1 + (mid >> LIMB_BITS) < 0
    return tuple(jnp.where(take, one, two) for one, two in zip(new, best))


def improve(best, new, bar):
    n1, n0, r1, r0, order = best
    m1, m0, s1, s0, index = new
    low = m0 * r0 - n0 * s0 + ((order - index) >> 31)
    mid = (m1 * r0 + m0 * r1) - (n1 * s0 + n0 * s1) + (low >> LIMB_BITS)
    take = m1 * r1 - n1 * s1 + (mid >> LIMB_BITS) >= bar
    return tuple(jnp.where(take, one, two) for one, two in zip(new, best))


def clear_margins(buffer):
    rows, width = buffer.shape
    buffer[:, 0:128] = jnp.zeros((rows, 128), jnp.float32)
    buffer[:, width - 128 :] = jnp.zeros((rows, 128), jnp.float32)


def pooled(window, weights):
    parts = []
    for block in window:
        head = block.astype(jnp.bfloat16)
        parts += [head, (block - head.astype(jnp.float32)).astype(jnp.bfloat16)]
    rows = window[0].shape[0]
    out = jnp.dot(jnp.concatenate(parts, axis=0), weights, preferred_element_type=jnp.float32)
    return [out[2 * b * rows : (2 * b + 1) * rows] + out[(2 * b + 1) * rows : (2 * b + 2) * rows] for b in range(len(window))]


def place():
    core = lax.axis_index("dates")
    z = lax.axis_index("rows")
    return jnp.where(core == 0, z > 0, z < lax.axis_size("rows") - 1), core


def inside(has, core, rows, near):
    index = lax.broadcasted_iota(jnp.int32, (rows, 128), 0)
    low = jnp.where(has | (core == 1), 0, near)
    high = jnp.where(has | (core == 0), rows, rows - near)
    return (index >= low) & (index < high)


def stacked(source, block, start, rows):
    value = TAPS[0] * source[block, pl.ds(start, rows, 2), :]
    for i in range(1, 6):
        value = value + TAPS[i] * source[block, pl.ds(start + i, rows, 2), :]
    return value


def descend(has, core, weights, source, start, rows, keep, near, out, padded, target):
    valid = inside(has, core, rows, near)
    blocks = source.shape[0] // 2
    for band in range(2):
        for c in range(blocks):
            value = stacked(source, band * blocks + c, start, rows)
            out[band, :, c * 128 : (c + 1) * 128] = value[keep : keep + out.shape[1]]
            padded[band * rows : (band + 1) * rows, 128 * (c + 1) : 128 * (c + 2)] = jnp.where(valid, value, 0.0)
    spans = blocks * 64 // SPAN
    results = pooled([padded[:, 2 * SPAN * b : 2 * SPAN * b + WINDOW] for b in range(spans)], weights[...])
    for b, result in enumerate(results):
        for band in range(2):
            for i in range(SPAN // 128):
                target[band * blocks // 2 + b * (SPAN // 128) + i, 0:rows] = result[
                    band * rows : (band + 1) * rows, i * 128 : (i + 1) * 128
                ]


def network(count):
    pairs, p = [], 1
    while p < count:
        k = p
        while k >= 1:
            for j in range(k % p, count - k, 2 * k):
                for i in range(j, j + min(k, count - j - k)):
                    if i // (2 * p) == (i + k) // (2 * p):
                        pairs.append((i, i + k))
            k //= 2
        p *= 2
    return pairs


def pieces_of(tiles, cols):
    widths = [4 * GROUP, 4 * GROUP, 4 * GROUP] + [cols] * (2 * tiles - 3)
    return [(slot, col, width) for slot, width in enumerate(widths) for col in range(0, cols, width)]


def kernel(
    ordinal_far, red, nir, cloud,
    comp, one, ext1, weights,
    ordinal, ranked, sent, got, mine, level, ext, level1,
    in_sem, ordinal_sem, send_sem, recv_sem, halo_send, halo_recv, *images
):
    dates, strip, cols = red.shape
    half = strip // 2
    tiles = half // TILE
    core = lax.axis_index("dates")
    z = lax.axis_index("rows")
    last = lax.axis_size("rows") - 1
    other = 1 - core
    has = jnp.where(core == 0, z > 0, z < last)
    beyond = jnp.where(core == 0, z - 1, z + 1)
    partner = {"dates": other}
    neighbour = {"rows": beyond, "dates": other}

    def tile_in_half(c, k):
        return jnp.where(c == 0, k, tiles - 1 - k)

    pieces = pieces_of(tiles, cols)

    def load(i):
        slot, start, width = pieces[i]
        owner = other if slot < tiles else core
        row = pl.multiple_of(owner * half + tile_in_half(owner, slot % tiles) * TILE, TILE)
        col = pl.ds(start, width)
        for j, src in enumerate((red, nir, cloud)):
            pltpu.make_async_copy(src.at[:, pl.ds(row, TILE), col], images[i].at[j], in_sem.at[i]).start()

    def loaded(i):
        pltpu.make_async_copy(images[i], images[i], in_sem.at[i]).wait()

    order_copy = pltpu.make_async_copy(ordinal_far, ordinal, ordinal_sem)
    order_copy.start()
    for i in range(len(pieces)):
        load(i)

    barrier = pltpu.get_barrier_semaphore()
    pl.semaphore_signal(barrier, inc=1, device_id=partner, device_id_type=MESH)

    @pl.when(has)
    def _():
        pl.semaphore_signal(barrier, inc=1, device_id=neighbour, device_id_type=MESH)

    shape = (WINDOW, SPAN)
    tap = lax.broadcasted_iota(jnp.int32, shape, 0) - 2 * lax.broadcasted_iota(jnp.int32, shape, 1) - 126
    factor = jnp.zeros(shape, jnp.float32)
    for i, weight in enumerate(TAPS):
        factor = jnp.where(tap == i, weight, factor)
    weights[...] = factor.astype(jnp.bfloat16)
    for buffer in (*(level.at[k] for k in range(tiles + 1)), level1):
        clear_margins(buffer)
    lanes = ext.shape[0]
    ext[:, 0:8] = jnp.zeros((lanes, 8, 128), jnp.float32)
    ext[:, 56:64] = jnp.zeros((lanes, 8, 128), jnp.float32)

    @pl.when(jnp.logical_not(has))
    def _():
        edge = pl.multiple_of(jnp.where(core == 0, 8, 40), 8)
        ext[:, pl.ds(edge, half)] = jnp.zeros((lanes, half, 128), jnp.float32)

    def best_of(image, col):
        product = image[2, 0, :, col]
        for d in range(1, dates):
            product = product * image[2, d, :, col]
        limit = jnp.where(product == 0, 0, CLEAR)
        best = None
        for d in range(dates):
            at = ranked[0, d]
            nir_value = jnp.where(image[2, at, :, col] > limit, 0, image[1, at, :, col])
            order = jnp.full((TILE, GROUP), ranked[1, d], jnp.int32)
            new = (*split(nir_value), *split(image[0, at, :, col]), order)
            best = new if best is None else younger(best, new)
        return best, product == 0

    def exchange(k, col):
        return pltpu.make_async_remote_copy(
            src_ref=sent.at[k, :, :, col],
            dst_ref=got.at[k, :, :, col],
            send_sem=send_sem,
            recv_sem=recv_sem.at[k],
            device_id=partner,
            device_id_type=MESH,
        )

    def columns(start, count):
        return [pl.ds(start + i * GROUP, GROUP) for i in range(count // GROUP)]

    def offer(best, is_clear, k, col):
        n1, n0, r1, r0, order = best
        sent[k, 0, :, col] = join(r1, r0)
        sent[k, 1, :, col] = join(n1, n0)
        sent[k, 2, :, col] = order + jnp.where(is_clear, FLAG_STEP, 0)

    order_copy.wait()
    keys = [(ordinal[d] << RADIX_BITS) + d for d in range(dates)]
    for i, j in network(dates):
        keys[i], keys[j] = jnp.minimum(keys[i], keys[j]), jnp.maximum(keys[i], keys[j])
    for d, key in enumerate(keys):
        ranked[0, d] = key & ((1 << RADIX_BITS) - 1)
        ranked[1, d] = key >> RADIX_BITS
    for i, (slot, start, width) in enumerate(pieces):
        if slot < tiles:
            loaded(i)
            for col, inner in zip(columns(start, width), columns(0, width)):
                offer(*best_of(images[i], inner), slot, col)
            if slot == 0 and start + width == cols:
                pl.semaphore_wait(barrier, jnp.where(has, 2, 1))
                exchange(slot, pl.ds(0, cols)).start()
            if slot > 0:
                exchange(slot, pl.ds(start, width)).start()

    for i, (slot, start, width) in enumerate(pieces):
        if slot >= tiles:
            loaded(i)
            for col, inner in zip(columns(start, width), columns(0, width)):
                best, is_clear = best_of(images[i], inner)
                for j, limb in enumerate((*best, jnp.where(is_clear, CLEAR, 0))):
                    mine[slot - tiles, j, :, col] = limb
                if slot == 2 * tiles - 1:
                    offer(best, is_clear, tiles, col)
    exchange(tiles, pl.ds(0, cols)).start()

    def halo(k, side):
        here = tile_in_half(core, k) * TILE
        there = 8 + 32 * (core if side == 0 else other) + here
        return pltpu.make_async_remote_copy(
            src_ref=ext.at[:, pl.ds(pl.multiple_of(24 + here, 8), TILE)],
            dst_ref=ext.at[:, pl.ds(pl.multiple_of(there, 8), TILE)],
            send_sem=halo_send.at[side],
            recv_sem=halo_recv.at[side],
            device_id=partner if side == 0 else neighbour,
            device_id_type=MESH,
        )

    def far_halo(c):
        here = (tiles - 1) * TILE if c == 0 else TILE - REACH
        there = 8 + 32 * (1 - c) + here
        return pltpu.make_async_remote_copy(
            src_ref=ext.at[:, 24 + here : 24 + here + REACH],
            dst_ref=ext.at[:, there : there + REACH],
            send_sem=halo_send.at[1],
            recv_sem=halo_recv.at[1],
            device_id=neighbour,
            device_id_type=MESH,
        )

    def unpack(packed, k, col):
        flagged = packed[k, 2, :, col]
        is_clear = flagged >= FLAG_STEP
        order = jnp.where(is_clear, flagged - FLAG_STEP, flagged)
        return (*split(packed[k, 1, :, col]), *split(packed[k, 0, :, col]), order), jnp.where(is_clear, CLEAR, 0)

    def fill(k, col, value_red, value_nir):
        inner = pl.ds(col.start + 128, GROUP)
        level[k, 0:8, inner] = value_red.astype(jnp.float32) * SCALE_BAND
        level[k, 8:16, inner] = value_nir.astype(jnp.float32) * SCALE_BAND

    def settle(k):
        row = pl.multiple_of(tile_in_half(core, k) * TILE, TILE)
        for col in columns(0, cols):
            theirs, fresh = unpack(got, k, col)
            bar = mine[k, 5, :, col] - fresh
            n1, n0, r1, r0, order = improve(tuple(mine[k, i, :, col] for i in range(5)), theirs, bar)
            value_red, value_nir = join(r1, r0), join(n1, n0)
            comp[0, pl.ds(row, TILE), col] = value_red
            comp[1, pl.ds(row, TILE), col] = value_nir
            comp[2, pl.ds(row, TILE), col] = order
            fill(k, col, value_red, value_nir)

    def settle_beside():
        for col in columns(0, cols):
            ours, clear = unpack(sent, tiles - 1, col)
            theirs, fresh = unpack(got, tiles, col)
            n1, n0, r1, r0, _ = improve(ours, theirs, clear - fresh)
            fill(tiles, col, join(r1, r0), join(n1, n0))

    def narrow(k, row):
        spans = cols // 2 // SPAN
        results = pooled([level[k, :, 2 * SPAN * b : 2 * SPAN * b + WINDOW] for b in range(spans)], weights[...])
        here = pl.ds(pl.multiple_of(row, 8), TILE)
        for b, result in enumerate(results):
            for i in range(SPAN // 128):
                piece = slice(i * 128, (i + 1) * 128)
                ext[b * (SPAN // 128) + i, here] = result[0:8, piece]
                ext[lanes // 2 + b * (SPAN // 128) + i, here] = result[8:16, piece]

    for k in range(tiles):
        pltpu.make_async_copy(got.at[k], got.at[k], recv_sem.at[k]).wait()
        settle(k)
        narrow(k, 24 + tile_in_half(core, k) * TILE)
        if k < tiles - 1:
            halo(k, 0).start()

        for c in range(2):

            @pl.when(has & (core == c))
            def _():
                (halo(k, 1) if k < tiles - 1 else far_halo(c)).start()

    pltpu.make_async_copy(got.at[tiles], got.at[tiles], recv_sem.at[tiles]).wait()
    settle_beside()
    narrow(tiles, 8 + 32 * other + tile_in_half(other, tiles - 1) * TILE)

    def settled(sems, side):
        rows = ext.at[:, 8 : 8 + half - TILE + (REACH if side == 1 else 0)]
        pltpu.make_async_copy(rows, rows, sems.at[side]).wait()

    settled(halo_recv, 0)

    @pl.when(has)
    def _():
        settled(halo_recv, 1)

    descend(has, core, weights, ext, 6, 24, 8, 8, one, level1, ext1)
    pltpu.make_async_copy(sent, sent, send_sem).wait()
    settled(halo_send, 0)

    @pl.when(has)
    def _():
        settled(halo_send, 1)


def finish(
    comp, one, ext1, weights,
    out_red, out_nir, out_chosen, out_one, out_two, out_three,
    two, three, level2, ext2, comp_sem, sems,
):
    pairs = ((one, out_one), (two, out_two), (three, out_three))
    copies = [pltpu.make_async_copy(src, dst, sems.at[i]) for i, (src, dst) in enumerate(pairs)]
    for i, out in enumerate((out_red, out_nir, out_chosen)):
        pltpu.make_async_copy(comp.at[i], out, comp_sem).start()
    copies[0].start()
    has, core = place()
    clear_margins(level2)
    descend(has, core, weights, ext1, 2, 8, 2, 2, two, level2, ext2)
    copies[1].start()
    blocks = ext2.shape[0] // 2
    for band in range(2):
        for c in range(blocks):
            three[band, :, c * 128 : (c + 1) * 128] = stacked(ext2, band * blocks + c, 0, 2)
    copies[2].start()
    for copy in copies:
        copy.wait()
    pltpu.make_async_copy(comp, comp, comp_sem).wait()


def body(red_band, nir_band, cloud_class, date_ordinal):
    dates, strip, cols = red_band.shape
    half = strip // 2
    tiles = half // TILE
    whole = pl.BlockSpec(memory_space=pltpu.VMEM)
    far = pl.BlockSpec(memory_space=pltpu.HBM)
    f32, i32 = jnp.float32, jnp.int32
    arrays = (date_ordinal, red_band, nir_band, cloud_class)
    arrays = [pltpu.with_memory_space_constraint(array, pltpu.HBM) for array in arrays]
    levels = [(2, half >> k, cols >> k) for k in (1, 2, 3)]
    near = pl.pallas_call(
        kernel,
        out_shape=[
            pltpu.VMEM((3, half, cols), i32),
            pltpu.VMEM(levels[0], f32),
            pltpu.VMEM((cols // 256, 24, 128), f32),
            pltpu.VMEM((WINDOW, SPAN), jnp.bfloat16),
        ],
        in_specs=[far] * 4,
        out_specs=[whole] * 4,
        scratch_shapes=[
            pltpu.SMEM((dates,), i32),
            pltpu.SMEM((2, dates), i32),
            pltpu.VMEM((tiles + 1, 3, TILE, cols), i32),
            pltpu.VMEM((tiles + 1, 3, TILE, cols), i32),
            pltpu.VMEM((tiles, 6, TILE, cols), i32),
            pltpu.VMEM((tiles + 1, 16, cols + 256), f32),
            pltpu.VMEM((cols // 128, 64, 128), f32),
            pltpu.VMEM((48, cols // 2 + 256), f32),
            pltpu.SemaphoreType.DMA((len(pieces_of(tiles, cols)),)),
            pltpu.SemaphoreType.DMA,
            pltpu.SemaphoreType.DMA,
            pltpu.SemaphoreType.DMA((tiles + 1,)),
            pltpu.SemaphoreType.DMA((2,)),
            pltpu.SemaphoreType.DMA((2,)),
        ]
        + [pltpu.VMEM((3, dates, TILE, width), i32) for _, _, width in pieces_of(tiles, cols)],
        compiler_params=pltpu.CompilerParams(
            collective_id=0, has_side_effects=True, vmem_limit_bytes=32 * 1024 * 1024
        ),
        name="composite",
    )(*arrays)
    return pl.pallas_call(
        finish,
        out_shape=[jax.ShapeDtypeStruct((half, cols), i32)] * 3 + [jax.ShapeDtypeStruct(shape, f32) for shape in levels],
        in_specs=[whole] * 4,
        out_specs=[far] * 6,
        scratch_shapes=[
            pltpu.VMEM(levels[1], f32),
            pltpu.VMEM(levels[2], f32),
            pltpu.VMEM((16, cols // 4 + 256), f32),
            pltpu.VMEM((cols // 512, 24, 128), f32),
            pltpu.SemaphoreType.DMA,
            pltpu.SemaphoreType.DMA((3,)),
        ],
        compiler_params=pltpu.CompilerParams(vmem_limit_bytes=16 * 1024 * 1024),
        name="finish",
    )(*near)


def solution(mesh):
    in_specs = (
        P("dates", ("tiles", "rows"), None),
        P("dates", ("tiles", "rows"), None),
        P("dates", ("tiles", "rows"), None),
        P(("tiles", "dates")),
    )
    out_specs = (
        P(("tiles", "rows", "dates"), None),
        P(("tiles", "rows", "dates"), None),
        P(("tiles", "rows", "dates"), None),
        P(None, ("tiles", "rows", "dates"), None),
        P(None, ("tiles", "rows", "dates"), None),
        P(None, ("tiles", "rows", "dates"), None),
    )
    return jax.shard_map(body, mesh=mesh, in_specs=in_specs, out_specs=out_specs, check_vma=False)
```
